32 devices in a mesh: dom: 8 (over z, core), grp: 4 (over y, x).
Axes of the slice: x: 2, y: 2, z: 4, core: 2. Of those that a mesh axis runs over, the one named last changes fastest.
Arguments:
- fine_level_residual: float32 [3, 15, 4096], P(None, None, ('dom', 'grp')), may hold values from -6 to 6
- restriction_matrix: float32 [3, 15], replicated, may hold values from -1.5 to 1.5
- prolongation_matrix: float32 [15, 3], replicated, may hold values from -3.5 to 3.5
- block_inverse: bfloat16 [9, 9, 4096], P(None, None, 'dom')
- face_coupling: bfloat16 [3, 9, 9, 4096], P(None, None, None, 'dom'), may hold values from -1.75 to 1.75
- neighbours: int32 [3, 4096], P(None, 'dom'), may hold values from -512 to 512, as said below
Outputs:
- correction: float32 [3, 15, 4096], P(None, None, ('dom', 'grp'))
The draws below stay inside these ranges and needn't reach their ends.
Inputs may be any that keep to these rules, and one draw needn't show every extreme that they name: `neighbours`: each entry is 0 or a nonzero offset d with |d| at most 512 such that e + d is another triangle of the grid.
All inputs are finite; a program needn't handle non-finite values.
Results may differ from the reference program's by a relative error of at most 0.0003.
Values sent between devices are 32-bit elements; how exact they have to be, the bound alone decides.
No kernel may reach another device: no remote copies, remote signals or barrier semaphores. Data moves between devices by JAX's collectives and lax.ppermute only.
A program may use at most 64 MiB of HBM per device.

```python
import jax
import jax.numpy as jnp
from jax import lax

EF = 128
SWEEPS = 6
ELEMS = 4096
N_GRP = 4


def draw_block_inverse(key, part):
    identity = jnp.eye(9, dtype=jnp.float32)[:, :, None]
    noise = jax.random.normal(jax.random.fold_in(key, 23), (9, 9, ELEMS), jnp.float32)
    value = 0.5 * identity + 0.08 * noise
    return value.astype(jnp.bfloat16)


def draw_neighbours(key, part):
    own = jnp.arange(ELEMS, dtype=jnp.int32)[None, :]
    reach = jax.random.randint(jax.random.fold_in(key, 31), (3, ELEMS), 1, EF * N_GRP + 1)
    direction = jax.random.randint(jax.random.fold_in(key, 32), (3, ELEMS), 0, 2) * 2 - 1
    offsets = reach * direction
    target = own + offsets
    wall = jax.random.randint(jax.random.fold_in(key, 33), (3, ELEMS), 0, 16) == 0
    inside = (target >= 0) & (target < ELEMS)
    return jnp.where(wall | jnp.logical_not(inside), 0, offsets).astype(jnp.int32)


def level_of(key, extent, shards, smallest, high):
    level = 1.0
    for dim, shards_of in shards:
        heights = jax.random.uniform(jax.random.fold_in(jax.random.fold_in(key, 6), dim), (shards_of,), jnp.float32, smallest / len(shards), high / len(shards))
        level = level * jnp.repeat(jnp.exp(heights), extent[dim] // shards_of).reshape((-1,) + (1,) * (len(extent) - 1 - dim))
    return level


def normal_values(key, shape, deviation, most, shards=(), kind=jnp.bfloat16):
    values = jax.random.normal(key, shape, jnp.float32) * deviation
    if len(shards) > 0:
        values = level_of(key, shape, shards, -0.22, 0.18) * values
    return jnp.clip(values, min=-most, max=most).astype(kind)


def setup_inputs(seed: int = 0) -> dict:
    keys = jax.random.split(jax.random.key(seed), 7)
    fine_level_residual = normal_values(keys[0], (3, 15, ELEMS), 1.0, 6.0, ((2, 32),), jnp.float32)
    restriction_matrix = normal_values(keys[1], (3, 15), 15 ** -0.5, 1.5, (), jnp.float32)
    prolongation_matrix = normal_values(keys[2], (15, 3), 3 ** -0.5, 3.5, (), jnp.float32)
    block_inverse = draw_block_inverse(jax.random.fold_in(keys[6], 71), 0)
    face_coupling = normal_values(keys[4], (3, 9, 9, ELEMS), 0.12, 1.75, ((3, 8),))
    neighbours = draw_neighbours(jax.random.fold_in(keys[6], 71), 0)
    return dict(fine_level_residual=fine_level_residual, restriction_matrix=restriction_matrix, prolongation_matrix=prolongation_matrix, block_inverse=block_inverse, face_coupling=face_coupling, neighbours=neighbours)


damping = 0.8


def one_sweep(current_iterate, coarse_forcing, block_inverse, face_coupling, neighbours):
    coupled = jnp.zeros_like(current_iterate)
    total = current_iterate.shape[1]
    own = jnp.arange(total, dtype=jnp.int32)
    for face_index in range(3):
        offsets = neighbours[face_index].astype(jnp.int32)
        position = jnp.clip(own + offsets, 0, total - 1).astype(jnp.int32)
        present = (offsets != 0).astype(jnp.float32)
        beside = current_iterate[:, position] * present[None, :]
        coupled = coupled + jnp.sum(face_coupling[face_index].astype(jnp.float32) * beside[None, :, :], axis=1)
    remain = coarse_forcing - coupled
    update = jnp.sum(block_inverse.astype(jnp.float32) * remain[None, :, :], axis=1)
    return (1.0 - damping) * current_iterate + damping * update


def reference(fine_level_residual, restriction_matrix, prolongation_matrix, block_inverse, face_coupling, neighbours):
    coarse_forcing = jnp.einsum("oc,acw->aow", restriction_matrix, fine_level_residual, precision=lax.Precision.HIGHEST)
    coarse_forcing = coarse_forcing.reshape(9, -1)
    current_iterate = jnp.zeros_like(coarse_forcing)
    for sweep_index in range(SWEEPS):
        current_iterate = one_sweep(current_iterate, coarse_forcing, block_inverse, face_coupling, neighbours)
    return jnp.einsum("oc,dcz->doz", prolongation_matrix, current_iterate.reshape(3, 3, -1), precision=lax.Precision.HIGHEST)
```

```python
import functools

import jax
import jax.numpy as jnp
from jax import lax
from jax.experimental import pallas as pl
from jax.experimental.pallas import tpu as pltpu
from jax.sharding import PartitionSpec as P

SWEEPS = 6
damping = 0.8
LANES = 128
SUBLANES = 8
COMP = 9
FACES = 3


class Shape:
    def __init__(self, width):
        self.W = width // LANES
        assert self.W * LANES == width and (self.W == 4 or self.W % 8 == 0)
        self.rows = -(-COMP * self.W // SUBLANES) * SUBLANES
        self.NV = self.rows // SUBLANES
        self.Q = max(1, self.W // SUBLANES)
        self.H = max(1, SUBLANES // self.W)
        self.reach = 2 * self.W + 1
        self.TS = 3 * self.W
        self.index_rows = max(SUBLANES, self.W)


def low_half():
    return lax.broadcasted_iota(jnp.int32, (SUBLANES, LANES), 0) < SUBLANES // 2


def restrict_kernel(residual_ref, restriction_ref, out_ref):
    nodes = residual_ref.shape[1]
    diagonal = lax.broadcasted_iota(jnp.int32, (nodes, nodes), 0) == lax.broadcasted_iota(
        jnp.int32, (nodes, nodes), 1
    )
    for m in range(3):
        row = jnp.broadcast_to(restriction_ref[m : m + 1, :], (nodes, nodes))
        column = jnp.sum(jnp.where(diagonal, row, 0.0), axis=1, keepdims=True)
        for v in range(3):
            out_ref[3 * v + m : 3 * v + m + 1, :] = jnp.sum(
                column * residual_ref[v], axis=0, keepdims=True
            )


def prepare_kernel(s, inverse_ref, coupling_ref, neighbours_ref, inv_out, coup_out, lane_out, rel_out):
    width = s.W * LANES
    pad = s.rows - COMP * s.W

    def unpack(matrix, out, where):
        for o in range(s.W):
            piece = matrix[:, o * LANES : (o + 1) * LANES]
            out[where + (pl.ds(o, SUBLANES, stride=s.W), slice(None))] = piece[:SUBLANES]
            out[where + (pl.ds(SUBLANES * s.W + o, 1), slice(None))] = piece[SUBLANES:COMP]
        if pad:
            out[where + (pl.ds(COMP * s.W, pad), slice(None))] = jnp.zeros((pad, LANES), jnp.float32)

    for i in range(COMP):
        unpack(inverse_ref[i].astype(jnp.float32), inv_out, (i,))
        for f in range(FACES):
            unpack(coupling_ref[f, i].astype(jnp.float32), coup_out, (f, i))
    lanes = lax.broadcasted_iota(jnp.int32, (1, LANES), 1)
    for f in range(FACES):
        for o in range(s.W):
            offset = neighbours_ref[f : f + 1, o * LANES : (o + 1) * LANES]
            position = lanes + offset + width
            lane = position & (LANES - 1)
            rel = jnp.where(offset == 0, -1, position >> 7)
            for h in range(s.H):
                row = h * s.W + o
                lane_out[f, row : row + 1, :] = lane
                rel_out[f, row : row + 1, :] = rel


def times(s, matrix, vectors):
    total = [[None] * s.Q for _ in range(COMP)]
    for i in range(COMP):
        for q in range(s.Q):
            acc = None
            for k, packed in enumerate(vectors):
                for v in range(q, s.NV, s.Q):
                    term = matrix(k, i, v) * packed[v]
                    acc = term if acc is None else acc + term
            total[i][q] = acc
    if s.H == 1:
        return [total[v // s.Q][v % s.Q] for v in range(s.NV)]
    low = low_half()
    out = []
    for v in range(s.NV):
        a = total[2 * v][0]
        b = total[2 * v + 1][0] if 2 * v + 1 < COMP else jnp.zeros_like(a)
        out.append(jnp.where(low, a, b) + pltpu.roll(jnp.where(low, b, a), s.W, 0))
    return out


def rows_of(ref, v):
    return ref[v * SUBLANES : (v + 1) * SUBLANES, :]


def first_kernel(s, slots, grp, inverse_ref, *refs):
    pieces, (rhs_out, iterate_out) = refs[:-2], refs[-2:]
    me = lax.axis_index(grp)
    if s.rows > COMP * s.W:
        pad = s.rows - COMP * s.W
        rhs_out[COMP * s.W :, :] = jnp.zeros((pad, LANES), jnp.float32)
    for k, piece in enumerate(pieces):
        slot = slots(me, k)
        rhs_out[pl.ds(slot, SUBLANES, stride=s.W), :] = piece[:SUBLANES, :]
        rhs_out[pl.ds(SUBLANES * s.W + slot, 1), :] = piece[SUBLANES:COMP, :]
    rhs = [rows_of(rhs_out, v) for v in range(s.NV)]
    update = times(s, lambda k, i, v: rows_of(inverse_ref.at[i], v), [rhs])
    for v in range(s.NV):
        iterate_out[v * SUBLANES : (v + 1) * SUBLANES, :] = damping * update[v]


def fill_table(s, table, block, place):
    for j in range(COMP):
        start = j * s.TS + place * s.W
        if s.H == 1:
            for q in range(s.Q):
                table[start + q * SUBLANES : start + (q + 1) * SUBLANES, :] = block[j * s.Q + q]
        else:
            half = (j % s.H) * s.W
            table[start : start + s.W, :] = block[j // s.H][half : half + s.W]


def sweep(s, dom, refs, table):
    inverse_ref, coupling_ref, lane_ref, rel_ref, rhs_ref, iterate_ref, even_ref, odd_ref = refs
    own = [rows_of(iterate_ref, v) for v in range(s.NV)]
    is_even = lax.rem(lax.axis_index(dom), 2) == 0
    pair = [rows_of(even_ref, v) for v in range(s.NV)]
    other = [rows_of(odd_ref, v) for v in range(s.NV)]
    fill_table(s, table, own, 1)
    fill_table(s, table, [jnp.where(is_even, o, p) for p, o in zip(pair, other)], 0)
    fill_table(s, table, [jnp.where(is_even, p, o) for p, o in zip(pair, other)], 2)
    table[COMP * s.TS :, :] = jnp.zeros((SUBLANES, LANES), jnp.float32)
    low = low_half()

    def source(v, r):
        if s.H == 1:
            start = (v // s.Q) * s.TS + (v % s.Q) * SUBLANES + r
            return table[start : start + SUBLANES, :]
        start = 2 * v * s.TS + r
        first = table[start : start + SUBLANES, :]
        if 2 * v + 1 >= COMP:
            return first
        start += s.TS - s.W
        return jnp.where(low, first, table[start : start + SUBLANES, :])

    lane = [[lane_ref[f, q * SUBLANES : (q + 1) * SUBLANES, :] for q in range(s.Q)] for f in range(FACES)]
    rel = [[rel_ref[f, q * SUBLANES : (q + 1) * SUBLANES, :] for q in range(s.Q)] for f in range(FACES)]
    beside = [[jnp.zeros((SUBLANES, LANES), jnp.float32)] * s.NV for _ in range(FACES)]
    for r in range(s.reach):
        here = [[rel[f][q] == r for q in range(s.Q)] for f in range(FACES)]
        for v in range(s.NV):
            tile = source(v, r)
            for f in range(FACES):
                taken = jnp.take_along_axis(tile, lane[f][v % s.Q], axis=1, mode="promise_in_bounds")
                beside[f][v] = jnp.where(here[f][v % s.Q], taken, beside[f][v])
    coupled = times(s, lambda f, i, v: rows_of(coupling_ref.at[f, i], v), beside)
    remain = [rows_of(rhs_ref, v) - coupled[v] for v in range(s.NV)]
    update = times(s, lambda k, i, v: rows_of(inverse_ref.at[i], v), [remain])
    return [(1.0 - damping) * own[v] + damping * update[v] for v in range(s.NV)]


def sweep_kernel(s, dom, *refs):
    out_ref, table = refs[-2:]
    new = sweep(s, dom, refs[:-2], table)
    for v in range(s.NV):
        out_ref[v * SUBLANES : (v + 1) * SUBLANES, :] = new[v]


def last_kernel(s, dom, grp, prolongation_ref, *refs):
    out_ref, table, final = refs[-3:]
    new = sweep(s, dom, refs[:-3], table)
    for v in range(s.NV):
        final[v * SUBLANES : (v + 1) * SUBLANES, :] = new[v]
    me = lax.axis_index(grp)
    rows = [final[pl.ds(j * s.W + me, 1), :] for j in range(COMP)]
    for v in range(3):
        acc = None
        for m in range(3):
            term = prolongation_ref[:, m : m + 1] * rows[3 * v + m]
            acc = term if acc is None else acc + term
        out_ref[v] = acc


def f32(*shape):
    return jax.ShapeDtypeStruct(shape, jnp.float32)


def call(kernel, name, out_shape, scratch=(), flops=0):
    return pl.pallas_call(
        kernel,
        out_shape=out_shape,
        scratch_shapes=scratch,
        compiler_params=pltpu.CompilerParams(vmem_limit_bytes=16 << 20),
        cost_estimate=pl.CostEstimate(flops=flops, bytes_accessed=0, transcendentals=0),
        name=name,
    )


def exchanges(n_dom, n_grp):
    out = []
    for first in (0, 1):
        partner = {d: d for d in range(n_dom)}
        for d in range(first, n_dom - 1, 2):
            partner[d], partner[d + 1] = d + 1, d
        perm = []
        for d in range(n_dom):
            for g in range(n_grp):
                to = g ^ 1 if partner[d] == d and n_grp % 2 == 0 else g
                perm.append((d * n_grp + g, partner[d] * n_grp + to))
        out.append(perm)
    return out


def local(n_dom, n_grp, fine_level_residual, restriction_matrix, prolongation_matrix, block_inverse, face_coupling, neighbours):
    s = Shape(block_inverse.shape[2])
    element_width = fine_level_residual.shape[2]
    assert element_width == LANES and s.W == n_grp
    own = call(restrict_kernel, "restrict", f32(COMP, LANES))(fine_level_residual, restriction_matrix)
    if n_grp & (n_grp - 1) == 0 and n_grp <= 4:
        pieces = [own] + [
            lax.ppermute(own, "grp", [(g, g ^ k) for g in range(n_grp)]) for k in range(1, n_grp)
        ]
        slots = lambda me, k: me ^ k
    else:
        gathered = lax.all_gather(own, "grp", axis=0)
        pieces = [gathered[k] for k in range(n_grp)]
        slots = lambda me, k: k
    inverse, coupling, lane, rel = call(
        functools.partial(prepare_kernel, s),
        "prepare",
        (
            f32(COMP, s.rows, LANES),
            f32(FACES, COMP, s.rows, LANES),
            jax.ShapeDtypeStruct((FACES, s.index_rows, LANES), jnp.int32),
            jax.ShapeDtypeStruct((FACES, s.index_rows, LANES), jnp.int32),
        ),
        flops=20_000_000,
    )(block_inverse, face_coupling, neighbours)
    rhs, iterate = call(
        functools.partial(first_kernel, s, slots, "grp"), "first", (f32(s.rows, LANES), f32(s.rows, LANES))
    )(inverse, *pieces)
    even, odd = exchanges(n_dom, n_grp)
    table = pltpu.VMEM((COMP * s.TS + SUBLANES, LANES), jnp.float32)
    for index in range(1, SWEEPS):
        pair = lax.ppermute(iterate, ("dom", "grp"), even)
        other = lax.ppermute(iterate, ("dom", "grp"), odd)
        operands = (inverse, coupling, lane, rel, rhs, iterate, pair, other)
        if index < SWEEPS - 1:
            iterate = call(
                functools.partial(sweep_kernel, s, "dom"), "sweep", f32(s.rows, LANES), (table,)
            )(*operands)
    return call(
        functools.partial(last_kernel, s, "dom", "grp"),
        "last",
        f32(3, prolongation_matrix.shape[0], LANES),
        (table, pltpu.VMEM((s.rows, LANES), jnp.float32)),
    )(prolongation_matrix, *operands)


def solution(mesh):
    placed = (
        P(None, None, ("dom", "grp")),
        P(),
        P(),
        P(None, None, "dom"),
        P(None, None, None, "dom"),
        P(None, "dom"),
    )
    return jax.shard_map(
        functools.partial(local, mesh.shape["dom"], mesh.shape["grp"]),
        mesh=mesh,
        in_specs=placed,
        out_specs=P(None, None, ("dom", "grp")),
        check_vma=False,
    )
```

```python
import functools

import jax
import jax.numpy as jnp
from jax import lax
from jax.experimental import pallas as pl
from jax.experimental.pallas import tpu as pltpu
from jax.sharding import PartitionSpec as P


SWEEPS = 6
damping = 0.8
LANES = 128
SUBLANES = 8
COMP = 9
FACES = 3


class Shape:
    def __init__(self, width):
        self.W = width // LANES
        assert self.W * LANES == width and (self.W == 4 or self.W % 8 == 0)
        self.rows = -(-COMP * self.W // SUBLANES) * SUBLANES
        self.NV = self.rows // SUBLANES
        self.Q = max(1, self.W // SUBLANES)
        self.H = max(1, SUBLANES // self.W)
        self.index_rows = max(SUBLANES, self.W)
        self.table_rows = 2 * COMP * self.W + 2 * SUBLANES if self.H == 1 else 2 * (self.rows + SUBLANES)


def place_of_row(s):
    row = lax.broadcasted_iota(jnp.int32, (SUBLANES, LANES), 0)
    return row & (s.W - 1) if s.H > 1 else row


def load(sources, targets, sems):
    copies = [
        pltpu.make_async_copy(source, target, sems.at[n]) for n, (source, target) in enumerate(zip(sources, targets))
    ]
    for copy in copies:
        copy.start()
    for copy in copies:
        copy.wait()


def restrict_kernel(residual_hbm, restriction_hbm, out_ref, residual_ref, restriction_ref, sems):
    load((residual_hbm, restriction_hbm), (residual_ref, restriction_ref), sems)
    nodes = residual_ref.shape[1]
    diagonal = lax.broadcasted_iota(jnp.int32, (nodes, nodes), 0) == lax.broadcasted_iota(
        jnp.int32, (nodes, nodes), 1
    )
    for m in range(3):
        row = jnp.broadcast_to(restriction_ref[m : m + 1, :], (nodes, nodes))
        column = jnp.sum(jnp.where(diagonal, row, 0.0), axis=1, keepdims=True)
        for v in range(3):
            out_ref[3 * v + m : 3 * v + m + 1, :] = jnp.sum(
                column * residual_ref[v], axis=0, keepdims=True
            )


def prepare_kernel(s, dom, *refs):
    sources, targets, sems = refs[:3], refs[-4:-1], refs[-1]
    inv_out, spread_out, coup_out, lane_out, own_out, halo_out, even_out = refs[3:-4]
    inverse_ref, coupling_ref, neighbours_ref = targets
    load(sources, targets, sems)
    width = s.W * LANES
    pad = s.rows - COMP * s.W
    zeros = jnp.zeros((max(pad, 1), LANES), jnp.float32)
    for i in range(COMP):
        matrix = inverse_ref[i].astype(jnp.float32)
        for o in range(s.W):
            piece = matrix[:, o * LANES : (o + 1) * LANES]
            inv_out[i, pl.ds(o, SUBLANES, stride=s.W), :] = piece[:SUBLANES]
            inv_out[i, SUBLANES * s.W + o : SUBLANES * s.W + o + 1, :] = piece[SUBLANES:COMP]
            for h in range(s.H):
                row = h * s.W + o
                spread_out[i, pl.ds(row, SUBLANES, stride=s.index_rows), :] = piece[:SUBLANES]
                row += SUBLANES * s.index_rows
                spread_out[i, row : row + 1, :] = piece[SUBLANES:COMP]
        if pad:
            inv_out[i, COMP * s.W :, :] = zeros
            for f in range(FACES):
                start = (f * COMP + i) * s.rows + COMP * s.W
                coup_out[start : start + pad, :] = zeros
        for j in range(COMP):
            matrix = coupling_ref[i, j].astype(jnp.float32)
            for o in range(s.W):
                coup_out[pl.ds(i * s.rows + j * s.W + o, FACES, stride=COMP * s.rows), :] = matrix[
                    :, o * LANES : (o + 1) * LANES
                ]
    lanes = lax.broadcasted_iota(jnp.int32, (1, LANES), 1)
    for f in range(FACES):
        for o in range(s.W):
            offset = neighbours_ref[f : f + 1, o * LANES : (o + 1) * LANES]
            position = lanes + offset + width
            reach = position >> 7
            tile = reach + o
            inside = (tile >= s.W) & (tile < 2 * s.W)
            wall = offset == 0
            lane = position & (LANES - 1)
            own = jnp.where(wall | ~inside, -1, reach & (s.W - 1))
            halo = jnp.where(wall | inside, -1, jnp.where(tile < s.W, reach, reach - s.W))
            for h in range(s.H):
                row = h * s.W + o
                lane_out[f, row : row + 1, :] = lane
                own_out[f, row : row + 1, :] = own
                halo_out[f, row : row + 1, :] = halo
    even_out[...] = jnp.full((SUBLANES, LANES), 1 - (lax.axis_index(dom) & 1), jnp.int32)


def rows_of(ref, v):
    return ref[v * SUBLANES : (v + 1) * SUBLANES, :]


def times(s, matrix, vectors):
    total = [[None] * s.Q for _ in range(COMP)]
    for i in range(COMP):
        for q in range(s.Q):
            acc = None
            for k, packed in enumerate(vectors):
                for v in range(q, s.NV, s.Q):
                    term = matrix(k, i, v) * packed[v]
                    acc = term if acc is None else acc + term
            total[i][q] = acc
    if s.H == 1:
        return [total[v // s.Q][v % s.Q] for v in range(s.NV)]
    low = lax.broadcasted_iota(jnp.int32, (SUBLANES, LANES), 0) < s.W
    out = []
    for v in range(s.NV):
        a = total[2 * v][0]
        b = total[2 * v + 1][0] if 2 * v + 1 < COMP else jnp.zeros_like(a)
        out.append(jnp.where(low, a, b) + pltpu.roll(jnp.where(low, b, a), s.W, 0))
    return out


def first_kernel(s, slots, grp, inverse_ref, *refs):
    pieces, (iterate_out, rhs_ref) = refs[:-2], refs[-2:]
    me = lax.axis_index(grp)
    if s.rows > COMP * s.W:
        rhs_ref[COMP * s.W :, :] = jnp.zeros((s.rows - COMP * s.W, LANES), jnp.float32)
    for k, piece in enumerate(pieces):
        slot = slots(me, k)
        rhs_ref[pl.ds(slot, SUBLANES, stride=s.W), :] = piece[:SUBLANES, :]
        rhs_ref[pl.ds(SUBLANES * s.W + slot, 1), :] = piece[SUBLANES:COMP, :]
    rhs = [rows_of(rhs_ref, v) for v in range(s.NV)]
    update = times(s, lambda k, i, v: rows_of(inverse_ref.at[i], v), [rhs])
    for v in range(s.NV):
        iterate_out[v * SUBLANES : (v + 1) * SUBLANES, :] = damping * update[v]


def fold_kernel(s, spread_ref, coupling_ref, out_ref):
    group = 3
    for q in range(s.Q):
        pairs = [(f, v) for f in range(FACES) for v in range(q, s.NV, s.Q)]
        for first in range(0, len(pairs), group):
            block = pairs[first : first + group]
            columns = [
                [
                    coupling_ref[(f * COMP + k) * s.rows + v * SUBLANES : (f * COMP + k) * s.rows + (v + 1) * SUBLANES, :]
                    for k in range(COMP)
                ]
                for f, v in block
            ]
            for i in range(COMP):
                acc = [None] * len(block)
                for k in range(COMP):
                    start = k * s.index_rows + q * SUBLANES
                    factor = spread_ref[i, start : start + SUBLANES, :]
                    for n in range(len(block)):
                        term = factor * columns[n][k]
                        acc[n] = term if acc[n] is None else acc[n] + term
                for n, (f, v) in enumerate(block):
                    out_ref[f, i, v * SUBLANES : (v + 1) * SUBLANES, :] = damping * acc[n]


def windows(s, table, low, high):
    if s.H == 1:
        for place, block in ((0, low), (1, high)):
            for v in range(s.NV):
                start = (v // s.Q) * 2 * s.W + place * s.W + (v % s.Q) * SUBLANES
                table[start : start + SUBLANES, :] = block[v]

        def source(v, k):
            start = (v // s.Q) * 2 * s.W + (v % s.Q) * SUBLANES + k
            return table[start : start + SUBLANES, :]

        return source
    top = s.rows + 2 * SUBLANES
    for v in range(s.NV):
        table[v * SUBLANES : (v + 1) * SUBLANES, :] = low[v]
        table[top + v * SUBLANES : top + (v + 1) * SUBLANES, :] = high[v]
    place = place_of_row(s)

    def source(v, k):
        if k == 0:
            return low[v]
        if k == s.W:
            return high[v]
        start = v * SUBLANES + k
        return jnp.where(
            place < s.W - k,
            table[start : start + SUBLANES, :],
            table[top + start - s.W : top + start - s.W + SUBLANES, :],
        )

    return source


def gathered(s, source, count, lane_ref, slot_ref):
    lane = [[lane_ref[f, q * SUBLANES : (q + 1) * SUBLANES, :] for q in range(s.Q)] for f in range(FACES)]
    slot = [[slot_ref[f, q * SUBLANES : (q + 1) * SUBLANES, :] for q in range(s.Q)] for f in range(FACES)]
    beside = [[jnp.zeros((SUBLANES, LANES), jnp.float32)] * s.NV for _ in range(FACES)]
    for k in range(count):
        here = [[slot[f][q] == k for q in range(s.Q)] for f in range(FACES)]
        for v in range(s.NV):
            tile = source(v, k)
            for f in range(FACES):
                taken = jnp.take_along_axis(tile, lane[f][v % s.Q], axis=1, mode="promise_in_bounds")
                beside[f][v] = jnp.where(here[f][v % s.Q], taken, beside[f][v])
    return beside


def own_kernel(s, folded_ref, lane_ref, slot_ref, constant_ref, iterate_ref, out_ref, table):
    own = [rows_of(iterate_ref, v) for v in range(s.NV)]
    beside = gathered(s, windows(s, table, own, own), s.W, lane_ref, slot_ref)
    coupled = times(s, lambda f, i, v: rows_of(folded_ref.at[f, i], v), beside)
    for v in range(s.NV):
        out_ref[v * SUBLANES : (v + 1) * SUBLANES, :] = (
            (1.0 - damping) * own[v] + rows_of(constant_ref, v) - coupled[v]
        )


def with_halo(s, folded_ref, lane_ref, slot_ref, even_ref, base_ref, near_ref, far_ref, table):
    even = even_ref[...] != 0
    near = [rows_of(near_ref, v) for v in range(s.NV)]
    far = [rows_of(far_ref, v) for v in range(s.NV)]
    low = [jnp.where(even, b, a) for a, b in zip(near, far)]
    high = [jnp.where(even, a, b) for a, b in zip(near, far)]
    beside = gathered(s, windows(s, table, low, high), s.W + 1, lane_ref, slot_ref)
    coupled = times(s, lambda f, i, v: rows_of(folded_ref.at[f, i], v), beside)
    return [rows_of(base_ref, v) - coupled[v] for v in range(s.NV)]


def halo_kernel(s, *refs):
    out_ref, table = refs[-2:]
    new = with_halo(s, *refs[:-2], table)
    for v in range(s.NV):
        out_ref[v * SUBLANES : (v + 1) * SUBLANES, :] = new[v]


def last_kernel(s, grp, prolongation_ref, *refs):
    out_ref, table, final = refs[-3:]
    new = with_halo(s, *refs[:-3], table)
    for v in range(s.NV):
        final[v * SUBLANES : (v + 1) * SUBLANES, :] = new[v]
    me = lax.axis_index(grp)
    rows = [final[pl.ds(j * s.W + me, 1), :] for j in range(COMP)]
    for v in range(3):
        acc = None
        for m in range(3):
            term = prolongation_ref[:, m : m + 1] * rows[3 * v + m]
            acc = term if acc is None else acc + term
        out_ref[v] = acc


def f32(*shape):
    return jax.ShapeDtypeStruct(shape, jnp.float32)


def i32(*shape):
    return jax.ShapeDtypeStruct(shape, jnp.int32)


def call(kernel, out_shape, scratch=(), flops=0):
    return pl.pallas_call(
        kernel,
        out_shape=out_shape,
        scratch_shapes=scratch,
        compiler_params=pltpu.CompilerParams(vmem_limit_bytes=16 << 20),
        cost_estimate=pl.CostEstimate(flops=flops, bytes_accessed=0, transcendentals=0),
    )


def call_loading(kernel, out_shape, operands, flops=0):
    return pl.pallas_call(
        kernel,
        out_shape=out_shape,
        in_specs=[pl.BlockSpec(memory_space=pl.ANY)] * len(operands),
        scratch_shapes=[pltpu.VMEM(x.shape, x.dtype) for x in operands]
        + [pltpu.SemaphoreType.DMA((len(operands),))],
        compiler_params=pltpu.CompilerParams(vmem_limit_bytes=16 << 20),
        cost_estimate=pl.CostEstimate(flops=flops, bytes_accessed=0, transcendentals=0),
    )(*[pltpu.with_memory_space_constraint(x, pltpu.MemorySpace.HBM) for x in operands])


def exchanges(n_dom, n_grp):
    out = []
    for first in (0, 1):
        partner = {d: d for d in range(n_dom)}
        for d in range(first, n_dom - 1, 2):
            partner[d], partner[d + 1] = d + 1, d
        perm = []
        for d in range(n_dom):
            for g in range(n_grp):
                to = g ^ 1 if partner[d] == d and n_grp % 2 == 0 else g
                perm.append((d * n_grp + g, partner[d] * n_grp + to))
        out.append(perm)
    return out


def uses_swaps(n_grp):
    return n_grp & (n_grp - 1) == 0 and n_grp <= 4


def swap_order(n_grp):
    return tuple(reversed(range(1, n_grp)))


def local(n_dom, n_grp, fine_level_residual, restriction_matrix, prolongation_matrix, block_inverse, face_coupling, neighbours):
    s = Shape(block_inverse.shape[2])
    element_width = fine_level_residual.shape[2]
    assert element_width == LANES and s.W == n_grp
    own = call_loading(restrict_kernel, f32(COMP, LANES), (fine_level_residual, restriction_matrix))
    if uses_swaps(n_grp):
        pieces = [own] + [None] * (n_grp - 1)
        for k in swap_order(n_grp):
            pieces[k] = lax.ppermute(own, "grp", [(g, g ^ k) for g in range(n_grp)])
        slots = lambda me, k: me ^ k
    else:
        all_own = lax.all_gather(own, "grp", axis=0)
        pieces = [all_own[k] for k in range(n_grp)]
        slots = lambda me, k: k
    index = i32(FACES, s.index_rows, LANES)
    inverse, spread, coupling, lane, own_slot, halo_slot, even = call_loading(
        functools.partial(prepare_kernel, s, "dom"),
        (
            f32(COMP, s.rows, LANES),
            f32(COMP, COMP * s.index_rows, LANES),
            f32(FACES * COMP * s.rows, LANES),
            index,
            index,
            index,
            i32(SUBLANES, LANES),
        ),
        (block_inverse, jnp.transpose(face_coupling, (1, 2, 0, 3)), neighbours),
        flops=10_000_000,
    )
    constant = call(
        functools.partial(first_kernel, s, slots, "grp"),
        f32(s.rows, LANES),
        (pltpu.VMEM((s.rows, LANES), jnp.float32),),
    )(inverse, *pieces)
    near_pairs, far_pairs = exchanges(n_dom, n_grp)
    table = pltpu.VMEM((s.table_rows, LANES), jnp.float32)
    iterate = constant
    for index in range(1, SWEEPS):
        far = lax.ppermute(iterate, ("dom", "grp"), far_pairs)
        near = lax.ppermute(iterate, ("dom", "grp"), near_pairs)
        if index == 1:
            folded = call(
                functools.partial(fold_kernel, s), f32(FACES, COMP, s.rows, LANES), flops=10_000_000
            )(spread, coupling)
        base = call(
            functools.partial(own_kernel, s), f32(s.rows, LANES), (table,), flops=10_000_000
        )(folded, lane, own_slot, constant, iterate)
        operands = (folded, lane, halo_slot, even, base, near, far)
        if index < SWEEPS - 1:
            iterate = call(functools.partial(halo_kernel, s), f32(s.rows, LANES), (table,))(*operands)
    return call(
        functools.partial(last_kernel, s, "grp"),
        f32(3, prolongation_matrix.shape[0], LANES),
        (table, pltpu.VMEM((s.rows, LANES), jnp.float32)),
    )(prolongation_matrix, *operands)


def solution(mesh):
    placed = (
        P(None, None, ("dom", "grp")),
        P(),
        P(),
        P(None, None, "dom"),
        P(None, None, None, "dom"),
        P(None, "dom"),
    )
    n_dom, n_grp = mesh.shape["dom"], mesh.shape["grp"]
    return jax.shard_map(
        functools.partial(local, n_dom, n_grp),
        mesh=mesh,
        in_specs=placed,
        out_specs=P(None, None, ("dom", "grp")),
        check_vma=False,
    )
```

```python
import functools

import jax
import jax.numpy as jnp
from jax import lax
from jax.experimental import pallas as pl
from jax.experimental.pallas import tpu as pltpu
from jax.sharding import PartitionSpec as P


SWEEPS = 6
damping = 0.8
LANES = 128
SUBLANES = 8
COMP = 9
FACES = 3


class Shape:
    def __init__(self, width):
        self.W = width // LANES
        assert self.W * LANES == width and (self.W == 4 or self.W % 8 == 0)
        self.rows = -(-COMP * self.W // SUBLANES) * SUBLANES
        self.NV = self.rows // SUBLANES
        self.Q = max(1, self.W // SUBLANES)
        self.H = max(1, SUBLANES // self.W)
        self.index_rows = max(SUBLANES, self.W)
        self.table_rows = 2 * COMP * self.W + 2 * SUBLANES if self.H == 1 else 2 * (self.rows + SUBLANES)


def place_of_row(s):
    row = lax.broadcasted_iota(jnp.int32, (SUBLANES, LANES), 0)
    return row & (s.W - 1) if s.H > 1 else row


def load(sources, targets, sems):
    copies = [
        pltpu.make_async_copy(source, target, sems.at[n]) for n, (source, target) in enumerate(zip(sources, targets))
    ]
    for copy in copies:
        copy.start()
    for copy in copies:
        copy.wait()


def restrict_kernel(residual_hbm, restriction_hbm, out_ref, residual_ref, restriction_ref, sems):
    load((residual_hbm, restriction_hbm), (residual_ref, restriction_ref), sems)
    nodes = residual_ref.shape[1]
    diagonal = lax.broadcasted_iota(jnp.int32, (nodes, nodes), 0) == lax.broadcasted_iota(
        jnp.int32, (nodes, nodes), 1
    )
    for m in range(3):
        row = jnp.broadcast_to(restriction_ref[m : m + 1, :], (nodes, nodes))
        column = jnp.sum(jnp.where(diagonal, row, 0.0), axis=1, keepdims=True)
        for v in range(3):
            out_ref[3 * v + m : 3 * v + m + 1, :] = jnp.sum(
                column * residual_ref[v], axis=0, keepdims=True
            )


def prepare_kernel(s, dom, *refs):
    sources, targets, sems = refs[:3], refs[-4:-1], refs[-1]
    inv_out, spread_out, coup_out, lane_out, own_out, halo_out, even_out = refs[3:-4]
    inverse_ref, coupling_ref, neighbours_ref = targets
    load(sources, targets, sems)
    width = s.W * LANES
    pad = s.rows - COMP * s.W
    zeros = jnp.zeros((max(pad, 1), LANES), jnp.float32)
    for i in range(COMP):
        matrix = inverse_ref[i].astype(jnp.float32)
        for o in range(s.W):
            piece = matrix[:, o * LANES : (o + 1) * LANES]
            inv_out[i, pl.ds(o, SUBLANES, stride=s.W), :] = piece[:SUBLANES]
            inv_out[i, SUBLANES * s.W + o : SUBLANES * s.W + o + 1, :] = piece[SUBLANES:COMP]
            for h in range(s.H):
                row = h * s.W + o
                spread_out[i, pl.ds(row, SUBLANES, stride=s.index_rows), :] = piece[:SUBLANES]
                row += SUBLANES * s.index_rows
                spread_out[i, row : row + 1, :] = piece[SUBLANES:COMP]
        if pad:
            inv_out[i, COMP * s.W :, :] = zeros
            for f in range(FACES):
                start = (f * COMP + i) * s.rows + COMP * s.W
                coup_out[start : start + pad, :] = zeros
        for j in range(COMP):
            matrix = coupling_ref[i, j].astype(jnp.float32)
            for o in range(s.W):
                coup_out[pl.ds(i * s.rows + j * s.W + o, FACES, stride=COMP * s.rows), :] = matrix[
                    :, o * LANES : (o + 1) * LANES
                ]
    lanes = lax.broadcasted_iota(jnp.int32, (1, LANES), 1)
    for f in range(FACES):
        for o in range(s.W):
            offset = neighbours_ref[f : f + 1, o * LANES : (o + 1) * LANES]
            position = lanes + offset + width
            reach = position >> 7
            tile = reach + o
            inside = (tile >= s.W) & (tile < 2 * s.W)
            wall = offset == 0
            lane = position & (LANES - 1)
            own = jnp.where(wall | ~inside, -1, reach & (s.W - 1))
            halo = jnp.where(wall | inside, -1, jnp.where(tile < s.W, reach, reach - s.W))
            for h in range(s.H):
                row = h * s.W + o
                lane_out[f, row : row + 1, :] = lane
                own_out[f, row : row + 1, :] = own
                halo_out[f, row : row + 1, :] = halo
    even_out[...] = jnp.full((SUBLANES, LANES), 1 - (lax.axis_index(dom) & 1), jnp.int32)


def rows_of(ref, v):
    return ref[v * SUBLANES : (v + 1) * SUBLANES, :]


def times(s, matrix, vectors):
    total = [[None] * s.Q for _ in range(COMP)]
    for i in range(COMP):
        for q in range(s.Q):
            acc = None
            for k, packed in enumerate(vectors):
                for v in range(q, s.NV, s.Q):
                    term = matrix(k, i, v) * packed[v]
                    acc = term if acc is None else acc + term
            total[i][q] = acc
    if s.H == 1:
        return [total[v // s.Q][v % s.Q] for v in range(s.NV)]
    low = lax.broadcasted_iota(jnp.int32, (SUBLANES, LANES), 0) < s.W
    out = []
    for v in range(s.NV):
        a = total[2 * v][0]
        b = total[2 * v + 1][0] if 2 * v + 1 < COMP else jnp.zeros_like(a)
        out.append(jnp.where(low, a, b) + pltpu.roll(jnp.where(low, b, a), s.W, 0))
    return out


def first_kernel(s, slots, grp, inverse_ref, *refs):
    pieces, (iterate_out, rhs_ref) = refs[:-2], refs[-2:]
    me = lax.axis_index(grp)
    if s.rows > COMP * s.W:
        rhs_ref[COMP * s.W :, :] = jnp.zeros((s.rows - COMP * s.W, LANES), jnp.float32)
    for k, piece in enumerate(pieces):
        slot = slots(me, k)
        rhs_ref[pl.ds(slot, SUBLANES, stride=s.W), :] = piece[:SUBLANES, :]
        rhs_ref[pl.ds(SUBLANES * s.W + slot, 1), :] = piece[SUBLANES:COMP, :]
    rhs = [rows_of(rhs_ref, v) for v in range(s.NV)]
    update = times(s, lambda k, i, v: rows_of(inverse_ref.at[i], v), [rhs])
    for v in range(s.NV):
        iterate_out[v * SUBLANES : (v + 1) * SUBLANES, :] = damping * update[v]


def fold_kernel(s, spread_ref, coupling_ref, out_ref):
    group = 3
    for q in range(s.Q):
        pairs = [(f, v) for f in range(FACES) for v in range(q, s.NV, s.Q)]
        for first in range(0, len(pairs), group):
            block = pairs[first : first + group]
            columns = [
                [
                    coupling_ref[(f * COMP + k) * s.rows + v * SUBLANES : (f * COMP + k) * s.rows + (v + 1) * SUBLANES, :]
                    for k in range(COMP)
                ]
                for f, v in block
            ]
            for i in range(COMP):
                acc = [None] * len(block)
                for k in range(COMP):
                    start = k * s.index_rows + q * SUBLANES
                    factor = spread_ref[i, start : start + SUBLANES, :]
                    for n in range(len(block)):
                        term = factor * columns[n][k]
                        acc[n] = term if acc[n] is None else acc[n] + term
                for n, (f, v) in enumerate(block):
                    out_ref[f, i, v * SUBLANES : (v + 1) * SUBLANES, :] = damping * acc[n]


def windows(s, table, low, high):
    if s.H == 1:
        for place, block in ((0, low), (1, high)):
            for v in range(s.NV):
                start = (v // s.Q) * 2 * s.W + place * s.W + (v % s.Q) * SUBLANES
                table[start : start + SUBLANES, :] = block[v]

        def source(v, k):
            start = (v // s.Q) * 2 * s.W + (v % s.Q) * SUBLANES + k
            return table[start : start + SUBLANES, :]

        return source
    top = s.rows + 2 * SUBLANES
    for v in range(s.NV):
        table[v * SUBLANES : (v + 1) * SUBLANES, :] = low[v]
        table[top + v * SUBLANES : top + (v + 1) * SUBLANES, :] = high[v]
    place = place_of_row(s)

    def source(v, k):
        if k == 0:
            return low[v]
        if k == s.W:
            return high[v]
        start = v * SUBLANES + k
        return jnp.where(
            place < s.W - k,
            table[start : start + SUBLANES, :],
            table[top + start - s.W : top + start - s.W + SUBLANES, :],
        )

    return source


def gathered(s, source, count, lane_ref, slot_ref):
    tiles = [[source(v, k) for v in range(s.NV)] for k in range(count)] if s.H > 1 else None
    beside = []
    for f in range(FACES):
        lane = [lane_ref[f, q * SUBLANES : (q + 1) * SUBLANES, :] for q in range(s.Q)]
        slot = [slot_ref[f, q * SUBLANES : (q + 1) * SUBLANES, :] for q in range(s.Q)]
        face = [jnp.zeros((SUBLANES, LANES), jnp.float32)] * s.NV
        for k in range(count):
            here = [slot[q] == k for q in range(s.Q)]
            for v in range(s.NV):
                tile = source(v, k) if tiles is None else tiles[k][v]
                taken = jnp.take_along_axis(tile, lane[v % s.Q], axis=1, mode="promise_in_bounds")
                face[v] = jnp.where(here[v % s.Q], taken, face[v])
        beside.append(face)
    return beside


def own_kernel(s, folded_ref, lane_ref, slot_ref, constant_ref, iterate_ref, out_ref, table):
    own = [rows_of(iterate_ref, v) for v in range(s.NV)]
    beside = gathered(s, windows(s, table, own, own), s.W, lane_ref, slot_ref)
    coupled = times(s, lambda f, i, v: rows_of(folded_ref.at[f, i], v), beside)
    for v in range(s.NV):
        out_ref[v * SUBLANES : (v + 1) * SUBLANES, :] = (
            (1.0 - damping) * own[v] + rows_of(constant_ref, v) - coupled[v]
        )


def with_halo(s, folded_ref, lane_ref, slot_ref, even_ref, base_ref, near_ref, far_ref, table):
    even = even_ref[...] != 0
    near = [rows_of(near_ref, v) for v in range(s.NV)]
    far = [rows_of(far_ref, v) for v in range(s.NV)]
    low = [jnp.where(even, b, a) for a, b in zip(near, far)]
    high = [jnp.where(even, a, b) for a, b in zip(near, far)]
    beside = gathered(s, windows(s, table, low, high), s.W + 1, lane_ref, slot_ref)
    coupled = times(s, lambda f, i, v: rows_of(folded_ref.at[f, i], v), beside)
    return [rows_of(base_ref, v) - coupled[v] for v in range(s.NV)]


def halo_kernel(s, *refs):
    out_ref, table = refs[-2:]
    new = with_halo(s, *refs[:-2], table)
    for v in range(s.NV):
        out_ref[v * SUBLANES : (v + 1) * SUBLANES, :] = new[v]


def last_kernel(s, grp, prolongation_ref, *refs):
    out_ref, table, final = refs[-3:]
    new = with_halo(s, *refs[:-3], table)
    for v in range(s.NV):
        final[v * SUBLANES : (v + 1) * SUBLANES, :] = new[v]
    me = lax.axis_index(grp)
    rows = [final[pl.ds(j * s.W + me, 1), :] for j in range(COMP)]
    for v in range(3):
        acc = None
        for m in range(3):
            term = prolongation_ref[:, m : m + 1] * rows[3 * v + m]
            acc = term if acc is None else acc + term
        out_ref[v] = acc


def f32(*shape):
    return jax.ShapeDtypeStruct(shape, jnp.float32)


def i32(*shape):
    return jax.ShapeDtypeStruct(shape, jnp.int32)


def call(kernel, out_shape, scratch=(), flops=0):
    return pl.pallas_call(
        kernel,
        out_shape=out_shape,
        scratch_shapes=scratch,
        compiler_params=pltpu.CompilerParams(vmem_limit_bytes=16 << 20),
        cost_estimate=pl.CostEstimate(flops=flops, bytes_accessed=0, transcendentals=0),
    )


def call_loading(kernel, out_shape, operands, flops=0):
    return pl.pallas_call(
        kernel,
        out_shape=out_shape,
        in_specs=[pl.BlockSpec(memory_space=pl.ANY)] * len(operands),
        scratch_shapes=[pltpu.VMEM(x.shape, x.dtype) for x in operands]
        + [pltpu.SemaphoreType.DMA((len(operands),))],
        compiler_params=pltpu.CompilerParams(vmem_limit_bytes=16 << 20),
        cost_estimate=pl.CostEstimate(flops=flops, bytes_accessed=0, transcendentals=0),
    )(*[pltpu.with_memory_space_constraint(x, pltpu.MemorySpace.HBM) for x in operands])


def exchanges(n_dom, n_grp):
    out = []
    for first in (0, 1):
        partner = {d: d for d in range(n_dom)}
        for d in range(first, n_dom - 1, 2):
            partner[d], partner[d + 1] = d + 1, d
        perm = []
        for d in range(n_dom):
            for g in range(n_grp):
                to = g ^ 1 if partner[d] == d and n_grp % 2 == 0 else g
                perm.append((d * n_grp + g, partner[d] * n_grp + to))
        out.append(perm)
    return out


def uses_swaps(n_grp):
    return n_grp & (n_grp - 1) == 0 and n_grp <= 4


def swap_order(n_grp):
    return tuple(reversed(range(1, n_grp)))


def local(n_dom, n_grp, fine_level_residual, restriction_matrix, prolongation_matrix, block_inverse, face_coupling, neighbours):
    s = Shape(block_inverse.shape[2])
    element_width = fine_level_residual.shape[2]
    assert element_width == LANES and s.W == n_grp
    own = call_loading(restrict_kernel, f32(COMP, LANES), (fine_level_residual, restriction_matrix))
    if uses_swaps(n_grp):
        pieces = [own] + [None] * (n_grp - 1)
        for k in swap_order(n_grp):
            pieces[k] = lax.ppermute(own, "grp", [(g, g ^ k) for g in range(n_grp)])
        slots = lambda me, k: me ^ k
    else:
        all_own = lax.all_gather(own, "grp", axis=0)
        pieces = [all_own[k] for k in range(n_grp)]
        slots = lambda me, k: k
    index = i32(FACES, s.index_rows, LANES)
    inverse, spread, coupling, lane, own_slot, halo_slot, even = call_loading(
        functools.partial(prepare_kernel, s, "dom"),
        (
            f32(COMP, s.rows, LANES),
            f32(COMP, COMP * s.index_rows, LANES),
            f32(FACES * COMP * s.rows, LANES),
            index,
            index,
            index,
            i32(SUBLANES, LANES),
        ),
        (block_inverse, jnp.transpose(face_coupling, (1, 2, 0, 3)), neighbours),
        flops=10_000_000,
    )
    constant = call(
        functools.partial(first_kernel, s, slots, "grp"),
        f32(s.rows, LANES),
        (pltpu.VMEM((s.rows, LANES), jnp.float32),),
    )(inverse, *pieces)
    near_pairs, far_pairs = exchanges(n_dom, n_grp)
    table = pltpu.VMEM((s.table_rows, LANES), jnp.float32)
    iterate = constant
    for index in range(1, SWEEPS):
        far = lax.ppermute(iterate, ("dom", "grp"), far_pairs)
        near = lax.ppermute(iterate, ("dom", "grp"), near_pairs)
        if index == 1:
            folded = call(
                functools.partial(fold_kernel, s), f32(FACES, COMP, s.rows, LANES), flops=10_000_000
            )(spread, coupling)
        base = call(
            functools.partial(own_kernel, s), f32(s.rows, LANES), (table,), flops=10_000_000
        )(folded, lane, own_slot, constant, iterate)
        operands = (folded, lane, halo_slot, even, base, near, far)
        if index < SWEEPS - 1:
            iterate = call(functools.partial(halo_kernel, s), f32(s.rows, LANES), (table,))(*operands)
    return call(
        functools.partial(last_kernel, s, "grp"),
        f32(3, prolongation_matrix.shape[0], LANES),
        (table, pltpu.VMEM((s.rows, LANES), jnp.float32)),
    )(prolongation_matrix, *operands)


def solution(mesh):
    placed = (
        P(None, None, ("dom", "grp")),
        P(),
        P(),
        P(None, None, "dom"),
        P(None, None, None, "dom"),
        P(None, "dom"),
    )
    n_dom, n_grp = mesh.shape["dom"], mesh.shape["grp"]
    return jax.shard_map(
        functools.partial(local, n_dom, n_grp),
        mesh=mesh,
        in_specs=placed,
        out_specs=P(None, None, ("dom", "grp")),
        check_vma=False,
    )
```

```python
import functools

import jax
import jax.numpy as jnp
from jax import lax
from jax.experimental import pallas as pl
from jax.experimental.pallas import tpu as pltpu
from jax.sharding import PartitionSpec as P


SWEEPS = 6
damping = 0.8
LANES = 128
SUBLANES = 8
COMP = 9
FACES = 3


class Shape:
    def __init__(self, width):
        self.W = width // LANES
        assert self.W * LANES == width and (self.W == 4 or self.W % 8 == 0)
        self.rows = -(-COMP * self.W // SUBLANES) * SUBLANES
        self.NV = self.rows // SUBLANES
        self.Q = max(1, self.W // SUBLANES)
        self.H = max(1, SUBLANES // self.W)
        self.index_rows = max(SUBLANES, self.W)
        self.table_rows = 2 * COMP * self.W + 2 * SUBLANES if self.H == 1 else 2 * (self.rows + SUBLANES)


def place_of_row(s):
    row = lax.broadcasted_iota(jnp.int32, (SUBLANES, LANES), 0)
    return row & (s.W - 1) if s.H > 1 else row


def load(sources, targets, sems):
    copies = [
        pltpu.make_async_copy(source, target, sems.at[n]) for n, (source, target) in enumerate(zip(sources, targets))
    ]
    for copy in copies:
        copy.start()
    for copy in copies:
        copy.wait()


def restrict_kernel(residual_hbm, restriction_hbm, out_ref, residual_ref, restriction_ref, sems):
    load((residual_hbm, restriction_hbm), (residual_ref, restriction_ref), sems)
    nodes = residual_ref.shape[1]
    diagonal = lax.broadcasted_iota(jnp.int32, (nodes, nodes), 0) == lax.broadcasted_iota(
        jnp.int32, (nodes, nodes), 1
    )
    for m in range(3):
        row = jnp.broadcast_to(restriction_ref[m : m + 1, :], (nodes, nodes))
        column = jnp.sum(jnp.where(diagonal, row, 0.0), axis=1, keepdims=True)
        for v in range(3):
            out_ref[3 * v + m : 3 * v + m + 1, :] = jnp.sum(
                column * residual_ref[v], axis=0, keepdims=True
            )


def prepare_kernel(s, dom, *refs):
    sources, targets, sems = refs[:3], refs[-4:-1], refs[-1]
    inv_out, spread_out, coup_out, lane_out, own_out, halo_out, even_out = refs[3:-4]
    inverse_ref, coupling_ref, neighbours_ref = targets
    load(sources, targets, sems)
    width = s.W * LANES
    pad = s.rows - COMP * s.W
    zeros = jnp.zeros((max(pad, 1), LANES), jnp.float32)
    for i in range(COMP):
        matrix = inverse_ref[i].astype(jnp.float32)
        for o in range(s.W):
            piece = matrix[:, o * LANES : (o + 1) * LANES]
            inv_out[i, pl.ds(o, SUBLANES, stride=s.W), :] = piece[:SUBLANES]
            inv_out[i, SUBLANES * s.W + o : SUBLANES * s.W + o + 1, :] = piece[SUBLANES:COMP]
            for h in range(s.H):
                row = h * s.W + o
                spread_out[i, pl.ds(row, SUBLANES, stride=s.index_rows), :] = piece[:SUBLANES]
                row += SUBLANES * s.index_rows
                spread_out[i, row : row + 1, :] = piece[SUBLANES:COMP]
        if pad:
            inv_out[i, COMP * s.W :, :] = zeros
            for f in range(FACES):
                start = (f * COMP + i) * s.rows + COMP * s.W
                coup_out[start : start + pad, :] = zeros
        for j in range(COMP):
            matrix = coupling_ref[i, j].astype(jnp.float32)
            for o in range(s.W):
                coup_out[pl.ds(i * s.rows + j * s.W + o, FACES, stride=COMP * s.rows), :] = matrix[
                    :, o * LANES : (o + 1) * LANES
                ]
    lanes = lax.broadcasted_iota(jnp.int32, (1, LANES), 1)
    for f in range(FACES):
        for o in range(s.W):
            offset = neighbours_ref[f : f + 1, o * LANES : (o + 1) * LANES]
            position = lanes + offset + width
            reach = position >> 7
            tile = reach + o
            inside = (tile >= s.W) & (tile < 2 * s.W)
            wall = offset == 0
            lane = position & (LANES - 1)
            own = jnp.where(wall | ~inside, -1, reach & (s.W - 1))
            halo = jnp.where(wall | inside, -1, jnp.where(tile < s.W, reach, reach - s.W))
            for h in range(s.H):
                row = h * s.W + o
                lane_out[f, row : row + 1, :] = lane
                own_out[f, row : row + 1, :] = own
                halo_out[f, row : row + 1, :] = halo
    even_out[...] = jnp.full((SUBLANES, LANES), 1 - (lax.axis_index(dom) & 1), jnp.int32)


def rows_of(ref, v):
    return ref[v * SUBLANES : (v + 1) * SUBLANES, :]


def times(s, matrix, vectors):
    total = [[None] * s.Q for _ in range(COMP)]
    for i in range(COMP):
        for q in range(s.Q):
            acc = None
            for k, packed in enumerate(vectors):
                for v in range(q, s.NV, s.Q):
                    term = matrix(k, i, v) * packed[v]
                    acc = term if acc is None else acc + term
            total[i][q] = acc
    if s.H == 1:
        return [total[v // s.Q][v % s.Q] for v in range(s.NV)]
    low = lax.broadcasted_iota(jnp.int32, (SUBLANES, LANES), 0) < s.W
    out = []
    for v in range(s.NV):
        a = total[2 * v][0]
        b = total[2 * v + 1][0] if 2 * v + 1 < COMP else jnp.zeros_like(a)
        out.append(jnp.where(low, a, b) + pltpu.roll(jnp.where(low, b, a), s.W, 0))
    return out


def first_kernel(s, slots, grp, inverse_ref, *refs):
    pieces, (iterate_out, rhs_ref) = refs[:-2], refs[-2:]
    me = lax.axis_index(grp)
    if s.rows > COMP * s.W:
        rhs_ref[COMP * s.W :, :] = jnp.zeros((s.rows - COMP * s.W, LANES), jnp.float32)
    for k, piece in enumerate(pieces):
        slot = slots(me, k)
        rhs_ref[pl.ds(slot, SUBLANES, stride=s.W), :] = piece[:SUBLANES, :]
        rhs_ref[pl.ds(SUBLANES * s.W + slot, 1), :] = piece[SUBLANES:COMP, :]
    rhs = [rows_of(rhs_ref, v) for v in range(s.NV)]
    update = times(s, lambda k, i, v: rows_of(inverse_ref.at[i], v), [rhs])
    for v in range(s.NV):
        iterate_out[v * SUBLANES : (v + 1) * SUBLANES, :] = damping * update[v]


def fold_kernel(s, spread_ref, coupling_ref, out_ref):
    group = 3
    for q in range(s.Q):
        pairs = [(f, v) for f in range(FACES) for v in range(q, s.NV, s.Q)]
        for first in range(0, len(pairs), group):
            block = pairs[first : first + group]
            columns = [
                [
                    coupling_ref[(f * COMP + k) * s.rows + v * SUBLANES : (f * COMP + k) * s.rows + (v + 1) * SUBLANES, :]
                    for k in range(COMP)
                ]
                for f, v in block
            ]
            for i in range(COMP):
                acc = [None] * len(block)
                for k in range(COMP):
                    start = k * s.index_rows + q * SUBLANES
                    factor = spread_ref[i, start : start + SUBLANES, :]
                    for n in range(len(block)):
                        term = factor * columns[n][k]
                        acc[n] = term if acc[n] is None else acc[n] + term
                for n, (f, v) in enumerate(block):
                    out_ref[f, i, v * SUBLANES : (v + 1) * SUBLANES, :] = damping * acc[n]


def windows(s, table, low, high):
    if s.H == 1:
        for place, block in ((0, low), (1, high)):
            for v in range(s.NV):
                start = (v // s.Q) * 2 * s.W + place * s.W + (v % s.Q) * SUBLANES
                table[start : start + SUBLANES, :] = block[v]

        def source(v, k):
            start = (v // s.Q) * 2 * s.W + (v % s.Q) * SUBLANES + k
            return table[start : start + SUBLANES, :]

        return source
    top = s.rows + 2 * SUBLANES
    for v in range(s.NV):
        table[v * SUBLANES : (v + 1) * SUBLANES, :] = low[v]
        table[top + v * SUBLANES : top + (v + 1) * SUBLANES, :] = high[v]
    place = place_of_row(s)

    def source(v, k):
        if k == 0:
            return low[v]
        if k == s.W:
            return high[v]
        start = v * SUBLANES + k
        return jnp.where(
            place < s.W - k,
            table[start : start + SUBLANES, :],
            table[top + start - s.W : top + start - s.W + SUBLANES, :],
        )

    return source


def gathered(s, source, count, lane_ref, slot_ref):
    tiles = [[source(v, k) for v in range(s.NV)] for k in range(count)] if s.H > 1 else None
    beside = []
    for f in range(FACES):
        lane = [lane_ref[f, q * SUBLANES : (q + 1) * SUBLANES, :] for q in range(s.Q)]
        slot = [slot_ref[f, q * SUBLANES : (q + 1) * SUBLANES, :] for q in range(s.Q)]
        face = [jnp.zeros((SUBLANES, LANES), jnp.float32)] * s.NV
        for k in range(count):
            here = [slot[q] == k for q in range(s.Q)]
            for v in range(s.NV):
                tile = source(v, k) if tiles is None else tiles[k][v]
                taken = jnp.take_along_axis(tile, lane[v % s.Q], axis=1, mode="promise_in_bounds")
                face[v] = jnp.where(here[v % s.Q], taken, face[v])
        beside.append(face)
    return beside


def own_kernel(s, folded_ref, lane_ref, slot_ref, constant_ref, iterate_ref, out_ref, table):
    own = [rows_of(iterate_ref, v) for v in range(s.NV)]
    beside = gathered(s, windows(s, table, own, own), s.W, lane_ref, slot_ref)
    coupled = times(s, lambda f, i, v: rows_of(folded_ref.at[f, i], v), beside)
    for v in range(s.NV):
        out_ref[v * SUBLANES : (v + 1) * SUBLANES, :] = (
            (1.0 - damping) * own[v] + rows_of(constant_ref, v) - coupled[v]
        )


def with_halo(s, folded_ref, lane_ref, slot_ref, even_ref, base_ref, near_ref, far_ref, table):
    even = even_ref[...] != 0
    near = [rows_of(near_ref, v) for v in range(s.NV)]
    far = [rows_of(far_ref, v) for v in range(s.NV)]
    low = [jnp.where(even, b, a) for a, b in zip(near, far)]
    high = [jnp.where(even, a, b) for a, b in zip(near, far)]
    beside = gathered(s, windows(s, table, low, high), s.W + 1, lane_ref, slot_ref)
    coupled = times(s, lambda f, i, v: rows_of(folded_ref.at[f, i], v), beside)
    return [rows_of(base_ref, v) - coupled[v] for v in range(s.NV)]


def halo_kernel(s, *refs):
    out_ref, table = refs[-2:]
    new = with_halo(s, *refs[:-2], table)
    for v in range(s.NV):
        out_ref[v * SUBLANES : (v + 1) * SUBLANES, :] = new[v]


def last_kernel(s, grp, prolongation_ref, *refs):
    out_ref, table, final = refs[-3:]
    new = with_halo(s, *refs[:-3], table)
    for v in range(s.NV):
        final[v * SUBLANES : (v + 1) * SUBLANES, :] = new[v]
    me = lax.axis_index(grp)
    rows = [final[pl.ds(j * s.W + me, 1), :] for j in range(COMP)]
    for v in range(3):
        acc = None
        for m in range(3):
            term = prolongation_ref[:, m : m + 1] * rows[3 * v + m]
            acc = term if acc is None else acc + term
        out_ref[v] = acc


def f32(*shape):
    return jax.ShapeDtypeStruct(shape, jnp.float32)


def i32(*shape):
    return jax.ShapeDtypeStruct(shape, jnp.int32)


def call(kernel, out_shape, scratch=(), flops=0):
    return pl.pallas_call(
        kernel,
        out_shape=out_shape,
        scratch_shapes=scratch,
        compiler_params=pltpu.CompilerParams(vmem_limit_bytes=16 << 20),
        cost_estimate=pl.CostEstimate(flops=flops, bytes_accessed=0, transcendentals=0),
    )


def call_loading(kernel, out_shape, operands, flops=0):
    return pl.pallas_call(
        kernel,
        out_shape=out_shape,
        in_specs=[pl.BlockSpec(memory_space=pl.ANY)] * len(operands),
        scratch_shapes=[pltpu.VMEM(x.shape, x.dtype) for x in operands]
        + [pltpu.SemaphoreType.DMA((len(operands),))],
        compiler_params=pltpu.CompilerParams(vmem_limit_bytes=16 << 20),
        cost_estimate=pl.CostEstimate(flops=flops, bytes_accessed=0, transcendentals=0),
    )(*[pltpu.with_memory_space_constraint(x, pltpu.MemorySpace.HBM) for x in operands])


def exchanges(n_dom, n_grp, fill):
    out = []
    for first in (0, 1):
        partner = {d: d for d in range(n_dom)}
        for d in range(first, n_dom - 1, 2):
            partner[d], partner[d + 1] = d + 1, d
        perm = []
        for d in range(n_dom):
            for g in range(n_grp):
                to = g ^ 1 if partner[d] == d and n_grp % 2 == 0 else g
                if fill or partner[d] != d:
                    perm.append((d * n_grp + g, partner[d] * n_grp + to))
        out.append(perm)
    return out


def uses_swaps(n_grp):
    return n_grp & (n_grp - 1) == 0 and n_grp <= 4


def swap_order(n_grp):
    return tuple(reversed(range(1, n_grp)))


def local(n_dom, n_grp, fine_level_residual, restriction_matrix, prolongation_matrix, block_inverse, face_coupling, neighbours):
    s = Shape(block_inverse.shape[2])
    element_width = fine_level_residual.shape[2]
    assert element_width == LANES and s.W == n_grp
    own = call_loading(restrict_kernel, f32(COMP, LANES), (fine_level_residual, restriction_matrix))
    if uses_swaps(n_grp):
        pieces = [own] + [None] * (n_grp - 1)
        for k in swap_order(n_grp):
            pieces[k] = lax.ppermute(own, "grp", [(g, g ^ k) for g in range(n_grp)])
        slots = lambda me, k: me ^ k
    else:
        all_own = lax.all_gather(own, "grp", axis=0)
        pieces = [all_own[k] for k in range(n_grp)]
        slots = lambda me, k: k
    index = i32(FACES, s.index_rows, LANES)
    inverse, spread, coupling, lane, own_slot, halo_slot, even = call_loading(
        functools.partial(prepare_kernel, s, "dom"),
        (
            f32(COMP, s.rows, LANES),
            f32(COMP, COMP * s.index_rows, LANES),
            f32(FACES * COMP * s.rows, LANES),
            index,
            index,
            index,
            i32(SUBLANES, LANES),
        ),
        (block_inverse, jnp.transpose(face_coupling, (1, 2, 0, 3)), neighbours),
        flops=10_000_000,
    )
    constant = call(
        functools.partial(first_kernel, s, slots, "grp"),
        f32(s.rows, LANES),
        (pltpu.VMEM((s.rows, LANES), jnp.float32),),
    )(inverse, *pieces)
    table = pltpu.VMEM((s.table_rows, LANES), jnp.float32)
    iterate = constant
    for index in range(1, SWEEPS):
        near_pairs, far_pairs = exchanges(n_dom, n_grp, index < SWEEPS - 1)
        far = lax.ppermute(iterate, ("dom", "grp"), far_pairs)
        near = lax.ppermute(iterate, ("dom", "grp"), near_pairs)
        if index == 1:
            folded = call(
                functools.partial(fold_kernel, s), f32(FACES, COMP, s.rows, LANES), flops=10_000_000
            )(spread, coupling)
        base = call(
            functools.partial(own_kernel, s), f32(s.rows, LANES), (table,), flops=10_000_000
        )(folded, lane, own_slot, constant, iterate)
        operands = (folded, lane, halo_slot, even, base, near, far)
        if index < SWEEPS - 1:
            iterate = call(functools.partial(halo_kernel, s), f32(s.rows, LANES), (table,))(*operands)
    return call(
        functools.partial(last_kernel, s, "grp"),
        f32(3, prolongation_matrix.shape[0], LANES),
        (table, pltpu.VMEM((s.rows, LANES), jnp.float32)),
    )(prolongation_matrix, *operands)


def solution(mesh):
    placed = (
        P(None, None, ("dom", "grp")),
        P(),
        P(),
        P(None, None, "dom"),
        P(None, None, None, "dom"),
        P(None, "dom"),
    )
    n_dom, n_grp = mesh.shape["dom"], mesh.shape["grp"]
    return jax.shard_map(
        functools.partial(local, n_dom, n_grp),
        mesh=mesh,
        in_specs=placed,
        out_specs=P(None, None, ("dom", "grp")),
        check_vma=False,
    )
```

```python
import functools

import jax
import jax.numpy as jnp
from jax import lax
from jax.experimental import pallas as pl
from jax.experimental.pallas import tpu as pltpu
from jax.sharding import PartitionSpec as P


SWEEPS = 6
damping = 0.8
LANES = 128
SUBLANES = 8
COMP = 9
FACES = 3


class Shape:
    def __init__(self, width):
        self.W = width // LANES
        assert self.W * LANES == width and (self.W == 4 or self.W % 8 == 0)
        self.rows = -(-COMP * self.W // SUBLANES) * SUBLANES
        self.NV = self.rows // SUBLANES
        self.Q = max(1, self.W // SUBLANES)
        self.H = max(1, SUBLANES // self.W)
        self.index_rows = max(SUBLANES, self.W)
        self.table_rows = 2 * COMP * self.W + 2 * SUBLANES if self.H == 1 else 2 * (self.rows + SUBLANES)


def place_of_row(s):
    row = lax.broadcasted_iota(jnp.int32, (SUBLANES, LANES), 0)
    return row & (s.W - 1) if s.H > 1 else row


def load(sources, targets, sems):
    copies = [
        pltpu.make_async_copy(source, target, sems.at[n]) for n, (source, target) in enumerate(zip(sources, targets))
    ]
    for copy in copies:
        copy.start()
    for copy in copies:
        copy.wait()


def restrict_kernel(grp, residual_hbm, restriction_hbm, inverse_hbm, out_ref, residual_ref, restriction_ref, inverse_ref, rhs_ref, sems):
    columns = pl.ds(pl.multiple_of(lax.axis_index(grp) * LANES, LANES), LANES)
    load(
        (residual_hbm, restriction_hbm, inverse_hbm.at[:, :, columns]),
        (residual_ref, restriction_ref, inverse_ref),
        sems,
    )
    nodes = residual_ref.shape[1]
    diagonal = lax.broadcasted_iota(jnp.int32, (nodes, nodes), 0) == lax.broadcasted_iota(
        jnp.int32, (nodes, nodes), 1
    )
    for m in range(3):
        row = jnp.broadcast_to(restriction_ref[m : m + 1, :], (nodes, nodes))
        column = jnp.sum(jnp.where(diagonal, row, 0.0), axis=1, keepdims=True)
        for v in range(3):
            rhs_ref[3 * v + m : 3 * v + m + 1, :] = jnp.sum(
                column * residual_ref[v], axis=0, keepdims=True
            )
    rhs = rhs_ref[...]
    for i in range(COMP):
        out_ref[i : i + 1, :] = damping * jnp.sum(
            inverse_ref[i].astype(jnp.float32) * rhs, axis=0, keepdims=True
        )


def prepare_kernel(s, dom, *refs):
    sources, targets, sems = refs[:3], refs[-4:-1], refs[-1]
    spread_out, coup_out, lane_out, own_out, halo_out, even_out = refs[3:-4]
    inverse_ref, coupling_ref, neighbours_ref = targets
    load(sources, targets, sems)
    width = s.W * LANES
    pad = s.rows - COMP * s.W
    zeros = jnp.zeros((max(pad, 1), LANES), jnp.float32)
    for i in range(COMP):
        matrix = inverse_ref[i].astype(jnp.float32)
        for o in range(s.W):
            piece = matrix[:, o * LANES : (o + 1) * LANES]
            for h in range(s.H):
                row = h * s.W + o
                spread_out[i, pl.ds(row, SUBLANES, stride=s.index_rows), :] = piece[:SUBLANES]
                row += SUBLANES * s.index_rows
                spread_out[i, row : row + 1, :] = piece[SUBLANES:COMP]
        if pad:
            for f in range(FACES):
                start = (f * COMP + i) * s.rows + COMP * s.W
                coup_out[start : start + pad, :] = zeros
        for j in range(COMP):
            matrix = coupling_ref[i, j].astype(jnp.float32)
            for o in range(s.W):
                coup_out[pl.ds(i * s.rows + j * s.W + o, FACES, stride=COMP * s.rows), :] = matrix[
                    :, o * LANES : (o + 1) * LANES
                ]
    lanes = lax.broadcasted_iota(jnp.int32, (1, LANES), 1)
    for f in range(FACES):
        for o in range(s.W):
            offset = neighbours_ref[f : f + 1, o * LANES : (o + 1) * LANES]
            position = lanes + offset + width
            reach = position >> 7
            tile = reach + o
            inside = (tile >= s.W) & (tile < 2 * s.W)
            wall = offset == 0
            lane = position & (LANES - 1)
            own = jnp.where(wall | ~inside, -1, reach & (s.W - 1))
            halo = jnp.where(wall | inside, -1, jnp.where(tile < s.W, reach, reach - s.W))
            for h in range(s.H):
                row = h * s.W + o
                lane_out[f, row : row + 1, :] = lane
                own_out[f, row : row + 1, :] = own
                halo_out[f, row : row + 1, :] = halo
    even_out[...] = jnp.full((SUBLANES, LANES), 1 - (lax.axis_index(dom) & 1), jnp.int32)


def rows_of(ref, v):
    return ref[v * SUBLANES : (v + 1) * SUBLANES, :]


def times(s, matrix, vectors):
    total = [[None] * s.Q for _ in range(COMP)]
    for i in range(COMP):
        for q in range(s.Q):
            acc = None
            for k, packed in enumerate(vectors):
                for v in range(q, s.NV, s.Q):
                    term = matrix(k, i, v) * packed[v]
                    acc = term if acc is None else acc + term
            total[i][q] = acc
    if s.H == 1:
        return [total[v // s.Q][v % s.Q] for v in range(s.NV)]
    low = lax.broadcasted_iota(jnp.int32, (SUBLANES, LANES), 0) < s.W
    out = []
    for v in range(s.NV):
        a = total[2 * v][0]
        b = total[2 * v + 1][0] if 2 * v + 1 < COMP else jnp.zeros_like(a)
        out.append(jnp.where(low, a, b) + pltpu.roll(jnp.where(low, b, a), s.W, 0))
    return out


def assemble_kernel(s, slots, grp, *refs):
    pieces, out_ref = refs[:-1], refs[-1]
    me = lax.axis_index(grp)
    if s.rows > COMP * s.W:
        out_ref[COMP * s.W :, :] = jnp.zeros((s.rows - COMP * s.W, LANES), jnp.float32)
    for k, piece in enumerate(pieces):
        slot = slots(me, k)
        out_ref[pl.ds(slot, SUBLANES, stride=s.W), :] = piece[:SUBLANES, :]
        out_ref[pl.ds(SUBLANES * s.W + slot, 1), :] = piece[SUBLANES:COMP, :]


def fold_kernel(s, spread_ref, coupling_ref, out_ref):
    group = 3
    for q in range(s.Q):
        pairs = [(f, v) for f in range(FACES) for v in range(q, s.NV, s.Q)]
        for first in range(0, len(pairs), group):
            block = pairs[first : first + group]
            columns = [
                [
                    coupling_ref[(f * COMP + k) * s.rows + v * SUBLANES : (f * COMP + k) * s.rows + (v + 1) * SUBLANES, :]
                    for k in range(COMP)
                ]
                for f, v in block
            ]
            for i in range(COMP):
                acc = [None] * len(block)
                for k in range(COMP):
                    start = k * s.index_rows + q * SUBLANES
                    factor = spread_ref[i, start : start + SUBLANES, :]
                    for n in range(len(block)):
                        term = factor * columns[n][k]
                        acc[n] = term if acc[n] is None else acc[n] + term
                for n, (f, v) in enumerate(block):
                    out_ref[f, i, v * SUBLANES : (v + 1) * SUBLANES, :] = damping * acc[n]


def windows(s, table, low, high):
    if s.H == 1:
        for place, block in ((0, low), (1, high)):
            for v in range(s.NV):
                start = (v // s.Q) * 2 * s.W + place * s.W + (v % s.Q) * SUBLANES
                table[start : start + SUBLANES, :] = block[v]

        def source(v, k):
            start = (v // s.Q) * 2 * s.W + (v % s.Q) * SUBLANES + k
            return table[start : start + SUBLANES, :]

        return source
    top = s.rows + 2 * SUBLANES
    for v in range(s.NV):
        table[v * SUBLANES : (v + 1) * SUBLANES, :] = low[v]
        table[top + v * SUBLANES : top + (v + 1) * SUBLANES, :] = high[v]
    place = place_of_row(s)

    def source(v, k):
        if k == 0:
            return low[v]
        if k == s.W:
            return high[v]
        start = v * SUBLANES + k
        return jnp.where(
            place < s.W - k,
            table[start : start + SUBLANES, :],
            table[top + start - s.W : top + start - s.W + SUBLANES, :],
        )

    return source


def gathered(s, source, count, lane_ref, slot_ref):
    tiles = [[source(v, k) for v in range(s.NV)] for k in range(count)] if s.H > 1 else None
    beside = []
    for f in range(FACES):
        lane = [lane_ref[f, q * SUBLANES : (q + 1) * SUBLANES, :] for q in range(s.Q)]
        slot = [slot_ref[f, q * SUBLANES : (q + 1) * SUBLANES, :] for q in range(s.Q)]
        face = [jnp.zeros((SUBLANES, LANES), jnp.float32)] * s.NV
        for k in range(count):
            here = [slot[q] == k for q in range(s.Q)]
            for v in range(s.NV):
                tile = source(v, k) if tiles is None else tiles[k][v]
                taken = jnp.take_along_axis(tile, lane[v % s.Q], axis=1, mode="promise_in_bounds")
                face[v] = jnp.where(here[v % s.Q], taken, face[v])
        beside.append(face)
    return beside


def own_kernel(s, folded_ref, lane_ref, slot_ref, constant_ref, iterate_ref, out_ref, table):
    own = [rows_of(iterate_ref, v) for v in range(s.NV)]
    beside = gathered(s, windows(s, table, own, own), s.W, lane_ref, slot_ref)
    coupled = times(s, lambda f, i, v: rows_of(folded_ref.at[f, i], v), beside)
    for v in range(s.NV):
        out_ref[v * SUBLANES : (v + 1) * SUBLANES, :] = (
            (1.0 - damping) * own[v] + rows_of(constant_ref, v) - coupled[v]
        )


def with_halo(s, folded_ref, lane_ref, slot_ref, even_ref, base_ref, near_ref, far_ref, table):
    even = even_ref[...] != 0
    near = [rows_of(near_ref, v) for v in range(s.NV)]
    far = [rows_of(far_ref, v) for v in range(s.NV)]
    low = [jnp.where(even, b, a) for a, b in zip(near, far)]
    high = [jnp.where(even, a, b) for a, b in zip(near, far)]
    beside = gathered(s, windows(s, table, low, high), s.W + 1, lane_ref, slot_ref)
    coupled = times(s, lambda f, i, v: rows_of(folded_ref.at[f, i], v), beside)
    return [rows_of(base_ref, v) - coupled[v] for v in range(s.NV)]


def halo_kernel(s, *refs):
    out_ref, table = refs[-2:]
    new = with_halo(s, *refs[:-2], table)
    for v in range(s.NV):
        out_ref[v * SUBLANES : (v + 1) * SUBLANES, :] = new[v]


def last_kernel(s, grp, prolongation_ref, *refs):
    out_ref, table, final = refs[-3:]
    new = with_halo(s, *refs[:-3], table)
    for v in range(s.NV):
        final[v * SUBLANES : (v + 1) * SUBLANES, :] = new[v]
    me = lax.axis_index(grp)
    rows = [final[pl.ds(j * s.W + me, 1), :] for j in range(COMP)]
    for v in range(3):
        acc = None
        for m in range(3):
            term = prolongation_ref[:, m : m + 1] * rows[3 * v + m]
            acc = term if acc is None else acc + term
        out_ref[v] = acc


def f32(*shape):
    return jax.ShapeDtypeStruct(shape, jnp.float32)


def i32(*shape):
    return jax.ShapeDtypeStruct(shape, jnp.int32)


def call(kernel, out_shape, scratch=(), flops=0):
    return pl.pallas_call(
        kernel,
        out_shape=out_shape,
        scratch_shapes=scratch,
        compiler_params=pltpu.CompilerParams(vmem_limit_bytes=16 << 20),
        cost_estimate=pl.CostEstimate(flops=flops, bytes_accessed=0, transcendentals=0),
    )


def call_loading(kernel, out_shape, operands, flops=0):
    return pl.pallas_call(
        kernel,
        out_shape=out_shape,
        in_specs=[pl.BlockSpec(memory_space=pl.ANY)] * len(operands),
        scratch_shapes=[pltpu.VMEM(x.shape, x.dtype) for x in operands]
        + [pltpu.SemaphoreType.DMA((len(operands),))],
        compiler_params=pltpu.CompilerParams(vmem_limit_bytes=16 << 20),
        cost_estimate=pl.CostEstimate(flops=flops, bytes_accessed=0, transcendentals=0),
    )(*[pltpu.with_memory_space_constraint(x, pltpu.MemorySpace.HBM) for x in operands])


def exchanges(n_dom, n_grp):
    out = []
    for first in (0, 1):
        partner = {d: d for d in range(n_dom)}
        for d in range(first, n_dom - 1, 2):
            partner[d], partner[d + 1] = d + 1, d
        perm = []
        for d in range(n_dom):
            for g in range(n_grp):
                to = g ^ 1 if partner[d] == d and n_grp % 2 == 0 else g
                perm.append((d * n_grp + g, partner[d] * n_grp + to))
        out.append(perm)
    return out


def uses_swaps(n_dom, n_grp):
    return n_dom % 2 == 0 and n_grp & (n_grp - 1) == 0 and n_grp <= 4


def swap_order(n_grp):
    return tuple(reversed(range(n_grp)))


def cross_swap(n_dom, n_grp, k):
    return [(d * n_grp + g, (d ^ 1) * n_grp + (g ^ k)) for d in range(n_dom) for g in range(n_grp)]


def cycle(n_dom, n_grp):
    following = {}
    for d in range(n_dom):
        to = d + 2 if d % 2 == 0 else d - 2
        following[d] = to if 0 <= to < n_dom else d ^ 1
    return [(d * n_grp + g, following[d] * n_grp + g) for d in range(n_dom) for g in range(n_grp)]


def local(n_dom, n_grp, fine_level_residual, restriction_matrix, prolongation_matrix, block_inverse, face_coupling, neighbours):
    s = Shape(block_inverse.shape[2])
    element_width = fine_level_residual.shape[2]
    assert element_width == LANES and s.W == n_grp
    hbm = lambda x: pltpu.with_memory_space_constraint(x, pltpu.MemorySpace.HBM)
    own = pl.pallas_call(
        functools.partial(restrict_kernel, "grp"),
        out_shape=f32(COMP, LANES),
        in_specs=[pl.BlockSpec(memory_space=pl.ANY)] * 3,
        scratch_shapes=[
            pltpu.VMEM(fine_level_residual.shape, jnp.float32),
            pltpu.VMEM(restriction_matrix.shape, jnp.float32),
            pltpu.VMEM((COMP, COMP, LANES), block_inverse.dtype),
            pltpu.VMEM((COMP, LANES), jnp.float32),
            pltpu.SemaphoreType.DMA((3,)),
        ],
        compiler_params=pltpu.CompilerParams(vmem_limit_bytes=16 << 20),
        name="restrict",
    )(hbm(fine_level_residual), hbm(restriction_matrix), hbm(block_inverse))
    crossed = uses_swaps(n_dom, n_grp)
    if crossed:
        pieces = [None] * n_grp
        for k in swap_order(n_grp):
            pieces[k] = lax.ppermute(own, ("dom", "grp"), cross_swap(n_dom, n_grp, k))
        slots = lambda me, k: me ^ k
    else:
        all_own = lax.all_gather(own, "grp", axis=0)
        pieces = [all_own[k] for k in range(n_grp)]
        slots = lambda me, k: k
    index = i32(FACES, s.index_rows, LANES)
    spread, coupling, lane, own_slot, halo_slot, even = call_loading(
        functools.partial(prepare_kernel, s, "dom"),
        (
            f32(COMP, COMP * s.index_rows, LANES),
            f32(FACES * COMP * s.rows, LANES),
            index,
            index,
            index,
            i32(SUBLANES, LANES),
        ),
        (block_inverse, jnp.transpose(face_coupling, (1, 2, 0, 3)), neighbours),
        flops=10_000_000,
    )
    folded = call(functools.partial(fold_kernel, s), f32(FACES, COMP, s.rows, LANES), flops=10_000_000)(
        spread, coupling
    )
    block = call(functools.partial(assemble_kernel, s, slots, "grp"), f32(s.rows, LANES))(*pieces)
    table = pltpu.VMEM((s.table_rows, LANES), jnp.float32)
    near_pairs, far_pairs = exchanges(n_dom, n_grp)
    constant = iterate = block
    for index in range(1, SWEEPS):
        swapped = crossed and index == 1
        far = lax.ppermute(iterate, ("dom", "grp"), cycle(n_dom, n_grp) if swapped else far_pairs)
        near = lax.ppermute(iterate, ("dom", "grp"), near_pairs)
        if swapped:
            constant = iterate = near
            near = block
        base = call(
            functools.partial(own_kernel, s), f32(s.rows, LANES), (table,), flops=10_000_000
        )(folded, lane, own_slot, constant, iterate)
        operands = (folded, lane, halo_slot, even, base, near, far)
        if index < SWEEPS - 1:
            iterate = call(functools.partial(halo_kernel, s), f32(s.rows, LANES), (table,))(*operands)
    return call(
        functools.partial(last_kernel, s, "grp"),
        f32(3, prolongation_matrix.shape[0], LANES),
        (table, pltpu.VMEM((s.rows, LANES), jnp.float32)),
    )(prolongation_matrix, *operands)


def solution(mesh):
    placed = (
        P(None, None, ("dom", "grp")),
        P(),
        P(),
        P(None, None, "dom"),
        P(None, None, None, "dom"),
        P(None, "dom"),
    )
    n_dom, n_grp = mesh.shape["dom"], mesh.shape["grp"]
    return jax.shard_map(
        functools.partial(local, n_dom, n_grp),
        mesh=mesh,
        in_specs=placed,
        out_specs=P(None, None, ("dom", "grp")),
        check_vma=False,
    )
```

```python
import functools

import jax
import jax.numpy as jnp
from jax import lax
from jax.experimental import pallas as pl
from jax.experimental.pallas import tpu as pltpu
from jax.sharding import PartitionSpec as P


SWEEPS = 6
damping = 0.8
LANES = 128
SUBLANES = 8
COMP = 9
FACES = 3


class Shape:
    def __init__(self, width):
        self.W = width // LANES
        assert self.W * LANES == width and (self.W == 4 or self.W % 8 == 0)
        self.rows = -(-COMP * self.W // SUBLANES) * SUBLANES
        self.NV = self.rows // SUBLANES
        self.Q = max(1, self.W // SUBLANES)
        self.H = max(1, SUBLANES // self.W)
        self.index_rows = max(SUBLANES, self.W)
        self.table_rows = 2 * COMP * self.W + 2 * SUBLANES if self.H == 1 else 2 * (self.rows + SUBLANES)


def place_of_row(s):
    row = lax.broadcasted_iota(jnp.int32, (SUBLANES, LANES), 0)
    return row & (s.W - 1) if s.H > 1 else row


def load(sources, targets, sems):
    copies = [
        pltpu.make_async_copy(source, target, sems.at[n]) for n, (source, target) in enumerate(zip(sources, targets))
    ]
    for copy in copies:
        copy.start()
    for copy in copies:
        copy.wait()


def restrict_kernel(grp, residual_hbm, restriction_hbm, inverse_hbm, out_ref, residual_ref, restriction_ref, inverse_ref, rhs_ref, sems):
    columns = pl.ds(pl.multiple_of(lax.axis_index(grp) * LANES, LANES), LANES)
    inverse_copy = pltpu.make_async_copy(inverse_hbm.at[:, :, columns], inverse_ref, sems.at[2])
    inverse_copy.start()
    load((residual_hbm, restriction_hbm), (residual_ref, restriction_ref), sems)
    nodes = residual_ref.shape[1]
    diagonal = lax.broadcasted_iota(jnp.int32, (nodes, nodes), 0) == lax.broadcasted_iota(
        jnp.int32, (nodes, nodes), 1
    )
    for m in range(3):
        row = jnp.broadcast_to(restriction_ref[m : m + 1, :], (nodes, nodes))
        column = jnp.sum(jnp.where(diagonal, row, 0.0), axis=1, keepdims=True)
        for v in range(3):
            rhs_ref[3 * v + m : 3 * v + m + 1, :] = jnp.sum(
                column * residual_ref[v], axis=0, keepdims=True
            )
    rhs = rhs_ref[...]
    inverse_copy.wait()
    for i in range(COMP):
        out_ref[i : i + 1, :] = damping * jnp.sum(
            inverse_ref[i].astype(jnp.float32) * rhs, axis=0, keepdims=True
        )


def prepare_kernel(s, dom, *refs):
    sources, targets, sems = refs[:3], refs[-4:-1], refs[-1]
    spread_out, coup_out, lane_out, own_out, halo_out, even_out = refs[3:-4]
    inverse_ref, coupling_ref, neighbours_ref = targets
    load(sources, targets, sems)
    width = s.W * LANES
    pad = s.rows - COMP * s.W
    zeros = jnp.zeros((max(pad, 1), LANES), jnp.float32)
    for i in range(COMP):
        matrix = inverse_ref[i].astype(jnp.float32)
        for o in range(s.W):
            piece = matrix[:, o * LANES : (o + 1) * LANES]
            for h in range(s.H):
                row = h * s.W + o
                spread_out[i, pl.ds(row, SUBLANES, stride=s.index_rows), :] = piece[:SUBLANES]
                row += SUBLANES * s.index_rows
                spread_out[i, row : row + 1, :] = piece[SUBLANES:COMP]
        if pad:
            for f in range(FACES):
                start = (f * COMP + i) * s.rows + COMP * s.W
                coup_out[start : start + pad, :] = zeros
        for j in range(COMP):
            matrix = coupling_ref[i, j].astype(jnp.float32)
            for o in range(s.W):
                coup_out[pl.ds(i * s.rows + j * s.W + o, FACES, stride=COMP * s.rows), :] = matrix[
                    :, o * LANES : (o + 1) * LANES
                ]
    lanes = lax.broadcasted_iota(jnp.int32, (1, LANES), 1)
    for f in range(FACES):
        for o in range(s.W):
            offset = neighbours_ref[f : f + 1, o * LANES : (o + 1) * LANES]
            position = lanes + offset + width
            reach = position >> 7
            tile = reach + o
            inside = (tile >= s.W) & (tile < 2 * s.W)
            wall = offset == 0
            lane = position & (LANES - 1)
            own = jnp.where(wall | ~inside, -1, reach & (s.W - 1))
            halo = jnp.where(wall | inside, -1, jnp.where(tile < s.W, reach, reach - s.W))
            for h in range(s.H):
                row = h * s.W + o
                lane_out[f, row : row + 1, :] = lane
                own_out[f, row : row + 1, :] = own
                halo_out[f, row : row + 1, :] = halo
    even_out[...] = jnp.full((SUBLANES, LANES), 1 - (lax.axis_index(dom) & 1), jnp.int32)


def rows_of(ref, v):
    return ref[v * SUBLANES : (v + 1) * SUBLANES, :]


def times(s, matrix, vectors):
    total = [[None] * s.Q for _ in range(COMP)]
    for i in range(COMP):
        for q in range(s.Q):
            acc = None
            for k, packed in enumerate(vectors):
                for v in range(q, s.NV, s.Q):
                    term = matrix(k, i, v) * packed[v]
                    acc = term if acc is None else acc + term
            total[i][q] = acc
    if s.H == 1:
        return [total[v // s.Q][v % s.Q] for v in range(s.NV)]
    low = lax.broadcasted_iota(jnp.int32, (SUBLANES, LANES), 0) < s.W
    out = []
    for v in range(s.NV):
        a = total[2 * v][0]
        b = total[2 * v + 1][0] if 2 * v + 1 < COMP else jnp.zeros_like(a)
        out.append(jnp.where(low, a, b) + pltpu.roll(jnp.where(low, b, a), s.W, 0))
    return out


def assemble_kernel(s, slots, grp, *refs):
    pieces, out_ref = refs[:-1], refs[-1]
    me = lax.axis_index(grp)
    if s.rows > COMP * s.W:
        out_ref[COMP * s.W :, :] = jnp.zeros((s.rows - COMP * s.W, LANES), jnp.float32)
    for k, piece in enumerate(pieces):
        slot = slots(me, k)
        out_ref[pl.ds(slot, SUBLANES, stride=s.W), :] = piece[:SUBLANES, :]
        out_ref[pl.ds(SUBLANES * s.W + slot, 1), :] = piece[SUBLANES:COMP, :]


def fold_kernel(s, spread_ref, coupling_ref, out_ref):
    group = 3
    for q in range(s.Q):
        pairs = [(f, v) for f in range(FACES) for v in range(q, s.NV, s.Q)]
        for first in range(0, len(pairs), group):
            block = pairs[first : first + group]
            columns = [
                [
                    coupling_ref[(f * COMP + k) * s.rows + v * SUBLANES : (f * COMP + k) * s.rows + (v + 1) * SUBLANES, :]
                    for k in range(COMP)
                ]
                for f, v in block
            ]
            for i in range(COMP):
                acc = [None] * len(block)
                for k in range(COMP):
                    start = k * s.index_rows + q * SUBLANES
                    factor = spread_ref[i, start : start + SUBLANES, :]
                    for n in range(len(block)):
                        term = factor * columns[n][k]
                        acc[n] = term if acc[n] is None else acc[n] + term
                for n, (f, v) in enumerate(block):
                    out_ref[f, i, v * SUBLANES : (v + 1) * SUBLANES, :] = damping * acc[n]


def windows(s, table, low, high):
    if s.H == 1:
        for place, block in ((0, low), (1, high)):
            for v in range(s.NV):
                start = (v // s.Q) * 2 * s.W + place * s.W + (v % s.Q) * SUBLANES
                table[start : start + SUBLANES, :] = block[v]

        def source(v, k):
            start = (v // s.Q) * 2 * s.W + (v % s.Q) * SUBLANES + k
            return table[start : start + SUBLANES, :]

        return source
    top = s.rows + 2 * SUBLANES
    for v in range(s.NV):
        table[v * SUBLANES : (v + 1) * SUBLANES, :] = low[v]
        table[top + v * SUBLANES : top + (v + 1) * SUBLANES, :] = high[v]
    place = place_of_row(s)

    def source(v, k):
        if k == 0:
            return low[v]
        if k == s.W:
            return high[v]
        start = v * SUBLANES + k
        return jnp.where(
            place < s.W - k,
            table[start : start + SUBLANES, :],
            table[top + start - s.W : top + start - s.W + SUBLANES, :],
        )

    return source


def gathered(s, source, count, lane_ref, slot_ref):
    tiles = [[source(v, k) for v in range(s.NV)] for k in range(count)] if s.H > 1 else None
    beside = []
    for f in range(FACES):
        lane = [lane_ref[f, q * SUBLANES : (q + 1) * SUBLANES, :] for q in range(s.Q)]
        slot = [slot_ref[f, q * SUBLANES : (q + 1) * SUBLANES, :] for q in range(s.Q)]
        face = [jnp.zeros((SUBLANES, LANES), jnp.float32)] * s.NV
        for k in range(count):
            here = [slot[q] == k for q in range(s.Q)]
            for v in range(s.NV):
                tile = source(v, k) if tiles is None else tiles[k][v]
                taken = jnp.take_along_axis(tile, lane[v % s.Q], axis=1, mode="promise_in_bounds")
                face[v] = jnp.where(here[v % s.Q], taken, face[v])
        beside.append(face)
    return beside


def own_kernel(s, folded_ref, lane_ref, slot_ref, constant_ref, iterate_ref, out_ref, table):
    own = [rows_of(iterate_ref, v) for v in range(s.NV)]
    beside = gathered(s, windows(s, table, own, own), s.W, lane_ref, slot_ref)
    coupled = times(s, lambda f, i, v: rows_of(folded_ref.at[f, i], v), beside)
    for v in range(s.NV):
        out_ref[v * SUBLANES : (v + 1) * SUBLANES, :] = (
            (1.0 - damping) * own[v] + rows_of(constant_ref, v) - coupled[v]
        )


def with_halo(s, folded_ref, lane_ref, slot_ref, even_ref, base_ref, near_ref, far_ref, table):
    even = even_ref[...] != 0
    near = [rows_of(near_ref, v) for v in range(s.NV)]
    far = [rows_of(far_ref, v) for v in range(s.NV)]
    low = [jnp.where(even, b, a) for a, b in zip(near, far)]
    high = [jnp.where(even, a, b) for a, b in zip(near, far)]
    beside = gathered(s, windows(s, table, low, high), s.W + 1, lane_ref, slot_ref)
    coupled = times(s, lambda f, i, v: rows_of(folded_ref.at[f, i], v), beside)
    return [rows_of(base_ref, v) - coupled[v] for v in range(s.NV)]


def halo_kernel(s, *refs):
    out_ref, table = refs[-2:]
    new = with_halo(s, *refs[:-2], table)
    for v in range(s.NV):
        out_ref[v * SUBLANES : (v + 1) * SUBLANES, :] = new[v]


def last_kernel(s, grp, prolongation_ref, *refs):
    out_ref, table, final = refs[-3:]
    new = with_halo(s, *refs[:-3], table)
    for v in range(s.NV):
        final[v * SUBLANES : (v + 1) * SUBLANES, :] = new[v]
    me = lax.axis_index(grp)
    rows = [final[pl.ds(j * s.W + me, 1), :] for j in range(COMP)]
    for v in range(3):
        acc = None
        for m in range(3):
            term = prolongation_ref[:, m : m + 1] * rows[3 * v + m]
            acc = term if acc is None else acc + term
        out_ref[v] = acc


def f32(*shape):
    return jax.ShapeDtypeStruct(shape, jnp.float32)


def i32(*shape):
    return jax.ShapeDtypeStruct(shape, jnp.int32)


def call(kernel, out_shape, scratch=(), flops=0):
    return pl.pallas_call(
        kernel,
        out_shape=out_shape,
        scratch_shapes=scratch,
        compiler_params=pltpu.CompilerParams(vmem_limit_bytes=16 << 20),
        cost_estimate=pl.CostEstimate(flops=flops, bytes_accessed=0, transcendentals=0),
    )


def call_loading(kernel, out_shape, operands, flops=0):
    return pl.pallas_call(
        kernel,
        out_shape=out_shape,
        in_specs=[pl.BlockSpec(memory_space=pl.ANY)] * len(operands),
        scratch_shapes=[pltpu.VMEM(x.shape, x.dtype) for x in operands]
        + [pltpu.SemaphoreType.DMA((len(operands),))],
        compiler_params=pltpu.CompilerParams(vmem_limit_bytes=16 << 20),
        cost_estimate=pl.CostEstimate(flops=flops, bytes_accessed=0, transcendentals=0),
    )(*[pltpu.with_memory_space_constraint(x, pltpu.MemorySpace.HBM) for x in operands])


def exchanges(n_dom, n_grp, fill):
    out = []
    for first in (0, 1):
        partner = {d: d for d in range(n_dom)}
        for d in range(first, n_dom - 1, 2):
            partner[d], partner[d + 1] = d + 1, d
        perm = []
        for d in range(n_dom):
            for g in range(n_grp):
                to = g ^ 1 if partner[d] == d and n_grp % 2 == 0 else g
                if fill or partner[d] != d:
                    perm.append((d * n_grp + g, partner[d] * n_grp + to))
        out.append(perm)
    return out


def uses_swaps(n_dom, n_grp):
    return n_dom % 2 == 0 and n_grp & (n_grp - 1) == 0 and n_grp <= 4


def swap_order(n_grp):
    return (*range(n_grp - 1, n_grp // 2, -1), *range(1, n_grp // 2 + 1), 0)


def cross_swap(n_dom, n_grp, k):
    return [(d * n_grp + g, (d ^ 1) * n_grp + (g ^ k)) for d in range(n_dom) for g in range(n_grp)]


def cycle(n_dom, n_grp):
    following = {}
    for d in range(n_dom):
        to = d + 2 if d % 2 == 0 else d - 2
        following[d] = to if 0 <= to < n_dom else d ^ 1
    return [(d * n_grp + g, following[d] * n_grp + g) for d in range(n_dom) for g in range(n_grp)]


def local(n_dom, n_grp, fine_level_residual, restriction_matrix, prolongation_matrix, block_inverse, face_coupling, neighbours):
    s = Shape(block_inverse.shape[2])
    element_width = fine_level_residual.shape[2]
    assert element_width == LANES and s.W == n_grp
    hbm = lambda x: pltpu.with_memory_space_constraint(x, pltpu.MemorySpace.HBM)
    own = pl.pallas_call(
        functools.partial(restrict_kernel, "grp"),
        out_shape=f32(COMP, LANES),
        in_specs=[pl.BlockSpec(memory_space=pl.ANY)] * 3,
        scratch_shapes=[
            pltpu.VMEM(fine_level_residual.shape, jnp.float32),
            pltpu.VMEM(restriction_matrix.shape, jnp.float32),
            pltpu.VMEM((COMP, COMP, LANES), block_inverse.dtype),
            pltpu.VMEM((COMP, LANES), jnp.float32),
            pltpu.SemaphoreType.DMA((3,)),
        ],
        compiler_params=pltpu.CompilerParams(vmem_limit_bytes=16 << 20),
        name="restrict",
    )(hbm(fine_level_residual), hbm(restriction_matrix), hbm(block_inverse))
    crossed = uses_swaps(n_dom, n_grp)
    if crossed:
        pieces = [None] * n_grp
        for k in swap_order(n_grp):
            pieces[k] = lax.ppermute(own, ("dom", "grp"), cross_swap(n_dom, n_grp, k))
        slots = lambda me, k: me ^ k
    else:
        all_own = lax.all_gather(own, "grp", axis=0)
        pieces = [all_own[k] for k in range(n_grp)]
        slots = lambda me, k: k
    index = i32(FACES, s.index_rows, LANES)
    spread, coupling, lane, own_slot, halo_slot, even = call_loading(
        functools.partial(prepare_kernel, s, "dom"),
        (
            f32(COMP, COMP * s.index_rows, LANES),
            f32(FACES * COMP * s.rows, LANES),
            index,
            index,
            index,
            i32(SUBLANES, LANES),
        ),
        (block_inverse, jnp.transpose(face_coupling, (1, 2, 0, 3)), neighbours),
        flops=10_000_000,
    )
    folded = call(functools.partial(fold_kernel, s), f32(FACES, COMP, s.rows, LANES), flops=10_000_000)(
        spread, coupling
    )
    block = call(functools.partial(assemble_kernel, s, slots, "grp"), f32(s.rows, LANES))(*pieces)
    table = pltpu.VMEM((s.table_rows, LANES), jnp.float32)
    constant = iterate = block
    for index in range(1, SWEEPS):
        swapped = crossed and index == 1
        near_pairs, far_pairs = exchanges(n_dom, n_grp, index < SWEEPS - 1)
        far = lax.ppermute(iterate, ("dom", "grp"), cycle(n_dom, n_grp) if swapped else far_pairs)
        near = lax.ppermute(iterate, ("dom", "grp"), near_pairs)
        if swapped:
            constant = iterate = near
            near = block
        base = call(
            functools.partial(own_kernel, s), f32(s.rows, LANES), (table,), flops=10_000_000
        )(folded, lane, own_slot, constant, iterate)
        operands = (folded, lane, halo_slot, even, base, near, far)
        if index < SWEEPS - 1:
            iterate = call(functools.partial(halo_kernel, s), f32(s.rows, LANES), (table,))(*operands)
    return call(
        functools.partial(last_kernel, s, "grp"),
        f32(3, prolongation_matrix.shape[0], LANES),
        (table, pltpu.VMEM((s.rows, LANES), jnp.float32)),
    )(prolongation_matrix, *operands)


def solution(mesh):
    placed = (
        P(None, None, ("dom", "grp")),
        P(),
        P(),
        P(None, None, "dom"),
        P(None, None, None, "dom"),
        P(None, "dom"),
    )
    n_dom, n_grp = mesh.shape["dom"], mesh.shape["grp"]
    return jax.shard_map(
        functools.partial(local, n_dom, n_grp),
        mesh=mesh,
        in_specs=placed,
        out_specs=P(None, None, ("dom", "grp")),
        check_vma=False,
    )
```
